512 devices in a mesh: row: 32 (over z, x), col: 16 (over y, core).
Axes of the slice: x: 4, y: 8, z: 8, core: 2. Of those that a mesh axis runs over, the one named last changes fastest.
Arguments:
- dense_a: bfloat16 [1024, 512, 512], P(('row', 'col')), may hold values from -6 to 6
- dense_b: bfloat16 [1024, 512, 512], P(('row', 'col')), may hold values from -0.25 to 0.25
- inner_basis_stack: bfloat16 [1024, 2, 512, 128], P(('row', 'col')), may hold values from -0.25 to 0.25
- outer_basis_stack: bfloat16 [1024, 2, 512, 128], P(('row', 'col')), may hold values from -1 to 1
- ascent: bfloat16 [512, 4, 2, 128, 128], P(('row', 'col')), may hold values from -0.4375 to 0.4375
- descent: bfloat16 [512, 4, 2, 128, 128], P(('row', 'col')), may hold values from -0.5 to 0.5
- couplings: bfloat16 [512, 2, 4, 128, 128], P(('row', 'col')), may hold values from -0.5 to 0.5
Outputs:
- product_diag: bfloat16 [1024, 512, 512], P(('row', 'col'))
The draws below stay inside these ranges and needn't reach their ends.
All inputs are finite; a program needn't handle non-finite values.
Results may differ from the reference program's by a relative error of at most 0.015.
Values may be sent and summed in bfloat16 or wider, within the bound.
A program may use at most 64 MiB of HBM per device.

```python
import jax
import jax.numpy as jnp
from jax import lax

M = 512
R = 128
DEVICES_ALL = 512
LEAVES = 1024
N_ROW = 32
N_COL = 16


def block_scale(rng, extent, shards, low, largest):
    level, own = 1.0, jax.random.fold_in(rng, 6)
    for position, shards_of in shards:
        draws = jnp.exp(jax.random.uniform(jax.random.fold_in(own, position), (shards_of,), jnp.float32, low / len(shards), largest / len(shards)))
        level = level * jnp.repeat(draws, extent[position] // shards_of).reshape([-1 if axis == position else 1 for axis in range(len(extent))])
    return level


def scatter_about(own_key, dims, width, reach, shards=(), kind=jnp.bfloat16):
    factor_of = block_scale(own_key, dims, shards, -0.22, 0.18) if shards else 1.0
    drawn = jax.random.normal(own_key, dims, jnp.float32) * width * factor_of
    return jnp.minimum(jnp.maximum(drawn, -reach), reach).astype(kind)


def setup_inputs(seed: int = 0) -> dict:
    keys = jax.random.split(jax.random.key(seed), 8)
    dense_a = scatter_about(keys[0], (LEAVES, M, M), 1.0, 6.0, ((0, 512),))
    dense_b = scatter_about(keys[1], (LEAVES, M, M), M ** -0.5, 0.25, ((0, 512),))
    inner_basis_stack = scatter_about(keys[2], (LEAVES, 2, M, R), M ** -0.5, 0.25, ((0, 512),))
    outer_basis_stack = scatter_about(keys[3], (LEAVES, 2, M, R), (R // 4) ** -0.5, 1.0, ((0, 512),))
    ascent = scatter_about(keys[4], (DEVICES_ALL, 4, 2, R, R), (R * 7 // 5) ** -0.5, 0.4375, ((0, 512),))
    descent = scatter_about(keys[5], (DEVICES_ALL, 4, 2, R, R), R ** -0.5, 0.5, ((0, 512),))
    couplings = scatter_about(keys[6], (DEVICES_ALL, 2, 4, R, R), R ** -0.5, 0.5, ((0, 512),))
    return {"dense_a": dense_a, "dense_b": dense_b, "inner_basis_stack": inner_basis_stack, "outer_basis_stack": outer_basis_stack, "ascent": ascent, "descent": descent, "couplings": couplings}


HIGHEST_PRECISION = lax.Precision.HIGHEST


def multiply(first_arg, second_arg):
    return jnp.matmul(first_arg.astype(jnp.float32), second_arg.astype(jnp.float32), precision=HIGHEST_PRECISION)


def lifted(pair_stack, inner_value):
    return multiply(multiply(jnp.swapaxes(pair_stack[:, 0], 1, 2), inner_value), pair_stack[:, 1])


def lowered(pair_stack, parent):
    return multiply(multiply(pair_stack[:, 0], parent), jnp.swapaxes(pair_stack[:, 1], 1, 2))


def sibling_terms(blocks, inner_value):
    left_terms = multiply(multiply(blocks[:, 0], inner_value[1::2]), blocks[:, 3])
    right_terms = multiply(multiply(blocks[:, 1], inner_value[0::2]), blocks[:, 2])
    return jnp.stack([left_terms, right_terms], 1).reshape(inner_value.shape)


def owners(stacked, height):
    return stacked[2 ** (height - 1) - 1::2 ** height]


def leaf_block(leaf_items):
    first_matrix_block, block_b, bases, mixing = leaf_items
    spread_rows = jnp.dot(bases[0], mixing, preferred_element_type=jnp.float32).astype(jnp.bfloat16)
    result_block = jnp.dot(first_matrix_block, block_b, preferred_element_type=jnp.float32)
    result_block = result_block + jnp.dot(spread_rows, bases[1].T, preferred_element_type=jnp.float32)
    return result_block.astype(jnp.bfloat16)


def reference(dense_a, dense_b, inner_basis_stack, outer_basis_stack, ascent, descent, couplings):
    device_list = N_ROW * N_COL
    levels = device_list.bit_length() - 1
    leaf_inner_product = jnp.einsum('ufw,ufa->uwa', inner_basis_stack[:, 0].astype(jnp.float32),
                            inner_basis_stack[:, 1].astype(jnp.float32), precision=HIGHEST_PRECISION)
    leaf_up = ascent[:, 0:2].reshape(2 * device_list, 2, R, R)
    inner_levels = [leaf_inner_product]
    lifted_terms = lifted(leaf_up, leaf_inner_product)
    current = lifted_terms[0::2] + lifted_terms[1::2]
    inner_levels.append(current)
    for height in range(1, levels + 1):
        if height == 1:
            pair_stack = ascent[:, 2]
        else:
            pair_stack = owners(ascent[:, 3], height - 1)
        lifted_terms = lifted(pair_stack, current)
        current = lifted_terms[0::2] + lifted_terms[1::2]
        inner_levels.append(current)
    coupling = jnp.zeros((1, R, R), jnp.float32)
    for height in range(levels, 0, -1):
        near_terms = sibling_terms(owners(couplings[:, 1], height), inner_levels[height])
        if height == 1:
            pair_stack = descent[:, 2]
        else:
            pair_stack = owners(descent[:, 3], height - 1)
        coupling = near_terms + lowered(pair_stack, jnp.repeat(coupling, 2, axis=0))
    near_terms = sibling_terms(couplings[:, 0], leaf_inner_product)
    leaf_down = descent[:, 0:2].reshape(2 * device_list, 2, R, R)
    leaf_coupling = near_terms + lowered(leaf_down, jnp.repeat(coupling, 2, axis=0))
    rounded_count = leaf_coupling.astype(jnp.bfloat16)
    return lax.map(leaf_block, (dense_a, dense_b, outer_basis_stack, rounded_count))
```

```python
import jax
import jax.numpy as jnp
from jax import lax
from jax.experimental import pallas as pl
from jax.experimental.pallas import tpu as pltpu
from jax.sharding import PartitionSpec as P

MESH_ID = pl.DeviceIdType.MESH
BF = jnp.bfloat16
F32 = jnp.float32
N_X = 4
N_Y = 8
N_Z = 8
TOP = 9


def flip1(p):
    return p + 1 - 2 * (p % 2)


def flip3(p):
    return p - p % 4 + 3 - p % 4


def halves(v):
    if v.dtype == BF:
        return (v,)
    high = v.astype(BF)
    return high, (v - high.astype(F32)).astype(BF)


def product(a, b, ca, cb):
    a, b = halves(a), halves(b)
    terms = [(i, j) for i in range(len(a)) for j in range(len(b)) if i + j < 2]
    if len(terms) == 1:
        left, right = a[0], b[0]
    else:
        left = jnp.concatenate([a[i] for i, _ in terms], ca)
        right = jnp.concatenate([b[j] for _, j in terms], cb)
    return lax.dot_general(left, right, (((ca,), (cb,)), ((), ())), preferred_element_type=F32)


def mm(a, b):
    return product(a, b, 1, 0)


def mm_t0(a, b):
    return product(a, b, 0, 0)


def mm_t1(a, b):
    return product(a, b, 1, 1)


def kernel(
    da, db, ib, ob, asc, desc, cp, out,
    va, vb, vib, vob, vasc, vdesc, vcp,
    acc, obuf, us, vw, s_f, s_t, r_f, r_t,
    t_pq, t_sw, t_k, low, top, s_fin, r_fin, s_g, r_g,
    ld_sem, st_sem, xs_sem, rf_sem, rt_sem, rpq_sem, rsw_sem, rk_sem,
    hs_sem, low_sem, top_sem, y_sem, tab_sem, fs_sem, fr_sem,
):
    row = lax.axis_index("row")
    col = lax.axis_index("col")
    z, x = row // N_X, row % N_X
    y, core = col // 2, col % 2

    loads = []
    pairs = ((ib, vib), (asc.at[0], vasc), (desc.at[0], vdesc), (cp.at[0], vcp), (ob, vob), (da, va), (db, vb))
    for i, (src, dst) in enumerate(pairs):
        c = pltpu.make_async_copy(src, dst, ld_sem.at[i])
        c.start()
        loads.append(c)

    barrier = pltpu.get_barrier_semaphore()

    def greet_plane(i, carry):
        r = (row + i // 2) % (N_X * N_Z)
        c = y * 2 + (core + i) % 2
        pl.semaphore_signal(barrier, inc=1, device_id=(r, c), device_id_type=MESH_ID)
        return carry

    lax.fori_loop(1, 2 * N_X * N_Z, greet_plane, 0)

    def greet_ring(i, carry):
        c = (col - core + i) % (2 * N_Y)
        pl.semaphore_signal(barrier, inc=1, device_id=(row, c), device_id_type=MESH_ID)
        return carry

    lax.fori_loop(2, 2 * N_Y, greet_ring, 0)

    with jax.named_scope("load"):
        loads[0].wait()
        loads[1].wait()
    leaf = [mm_t0(vib[i, 0], vib[i, 1]) for i in range(2)]
    term = [mm(mm_t0(vasc[i, 0], leaf[i]), vasc[i, 1]) for i in range(2)]
    node = term[0] + term[1]
    lifted = mm(mm_t0(vasc[2, 0], node), vasc[2, 1])
    s_f[1] = node.astype(BF)
    s_t[1] = lifted.astype(BF)

    with jax.named_scope("entry"):
        pl.semaphore_wait(barrier, 2 * N_X * N_Z - 1 + 2 * N_Y - 2)

    def remote(src, dst, ssem, rsem, r, c):
        return pltpu.make_async_remote_copy(
            src_ref=src, dst_ref=dst, send_sem=ssem, recv_sem=rsem,
            device_id=(r, c), device_id_type=MESH_ID,
        )

    def arrived(dst, sem, name="wait"):
        with jax.named_scope(name):
            remote(dst, dst, xs_sem.at[0, 0], sem, row, col).wait_recv()

    def dense(i, r):
        rows = pl.ds(r * 128, 128)
        acc[i, rows, :] = jnp.dot(va[i, rows, :], vb[i], preferred_element_type=F32)

    def side_terms(kl1, kr1):
        near_node = mm(mm(kl1, r_f[1]), kr1)
        for i in range(2):
            kl, kr = (vcp[0, 0], vcp[0, 3]) if i == 0 else (vcp[0, 1], vcp[0, 2])
            g = mm(mm(kl, leaf[1 - i]), kr)
            g = g + mm_t1(mm(vdesc[i, 0], near_node), vdesc[i, 1])
            us[i] = mm(vob[i, 0], mm(vdesc[i, 0], vdesc[2, 0])).astype(BF)
            vw[i] = mm(vob[i, 1], mm(vdesc[i, 1], vdesc[2, 1])).astype(BF)
            acc[i] += mm_t1(mm(vob[i, 0], g.astype(BF)).astype(BF), vob[i, 1])

    def finish(g, left, right):
        arrived(r_f.at[TOP], rf_sem.at[TOP], "wait_f9")
        g = (g + mm(mm(left, r_f[TOP]), right)).astype(BF)
        stores = []
        for i in range(2):
            spread = mm(us[i], g).astype(BF)
            for r in range(2):
                rows = pl.ds(r * 256, 256)
                block = acc[i, rows, :] + mm_t1(spread[r * 256:(r + 1) * 256], vw[i])
                obuf[i, rows, :] = block.astype(BF)
                c = pltpu.make_async_copy(obuf.at[i, rows], out.at[i, rows], st_sem.at[2 * i + r])
                c.start()
                stores.append(c)
        with jax.named_scope("stores"):
            for c in stores:
                c.wait()

    def route(h):
        p = {2: y, 3: y, 4: y, 5: x, 6: x, 7: z, 8: z, 9: z}[h]
        if h in (2, 5, 7):
            return None, flip1(p), None
        if h == 6:
            return None, 3 - p, None
        middle = ((p + 1) // 2) % 2
        if h in (3, 8):
            near = flip3(p)
            return middle == 1, near, flip1(near)
        near = 7 - p
        return middle == 0, near, flip1(near)

    def place(h, p, c):
        if h <= 4:
            return row, p * 2 + c
        if h <= 6:
            return z * N_X + p, y * 2 + c
        return p * N_X + x, y * 2 + c

    def when(cond, f):
        if cond is None:
            f()
        else:
            pl.when(cond)(f)

    def send_f(h, p, c, k):
        r, cc = place(h, p, c)
        return remote(s_f.at[h], r_f.at[h], xs_sem.at[h, k], rf_sem.at[h], r, cc)

    def send_t(h, p, k):
        r, cc = place(h, p, 1)
        return remote(s_t.at[h], r_t.at[h], xs_sem.at[h, k], rt_sem.at[h], r, cc)

    def table_copies(src, h, r, c, side, i):
        return (
            lambda: (remote(src.at[pl.ds(0, 2)], t_pq.at[h], tab_sem.at[0, i], rpq_sem.at[h], r, c),),
            lambda: (remote(src.at[pl.ds(2, 2)], t_sw.at[h], tab_sem.at[1, i], rsw_sem.at[h], r, c),),
            lambda: (
                remote(src.at[4 + side], t_k.at[h, 0], tab_sem.at[2, i], rk_sem.at[h, 0], r, c),
                remote(src.at[7 - side], t_k.at[h, 1], tab_sem.at[3, i], rk_sem.at[h, 1], r, c),
            ),
        )

    @pl.when(core == 1)
    def _():
        me_c = y * 2 + 1
        send = remote(s_f.at[1], r_f.at[1], xs_sem.at[1, 0], rf_sem.at[1], row, me_c - 1)
        send.start()
        loads[2].wait()
        loads[3].wait()

        def hand_over(dst, sems):
            return [
                remote(vasc.at[3], dst.at[pl.ds(0, 2)], hs_sem.at[0], sems.at[0], row, me_c - 1),
                remote(vdesc.at[3], dst.at[pl.ds(2, 2)], hs_sem.at[1], sems.at[1], row, me_c - 1),
                remote(vcp.at[1], dst.at[pl.ds(4, 4)], hs_sem.at[2], sems.at[2], row, me_c - 1),
            ]

        @pl.when(y == 7)
        def _():
            for c in hand_over(top, top_sem):
                c.start()

        @pl.when(y != 7)
        def _():
            for c in hand_over(low, low_sem):
                c.start()

        down = {}

        def compose(h):
            arrived(t_k.at[h, 0], rk_sem.at[h, 0], f"wait_k{h}")
            arrived(t_k.at[h, 1], rk_sem.at[h, 1], f"wait_k{h}")
            left, right = t_k[h, 0], t_k[h, 1]
            if h >= 3:
                arrived(t_sw.at[h - 2], rsw_sem.at[h - 2], f"wait_sw{h - 2}")
                s, w = t_sw[h - 2, 0], t_sw[h - 2, 1]
                if h == 3:
                    down["s"], down["w"] = s, w.T
                else:
                    down["s"] = mm(down["s"], s)
                    down["w"] = mm_t0(w, down["w"])
                left = mm(down["s"], left)
                right = mm(right, down["w"])
            if h == TOP:
                return left, right
            g = mm(mm(left, r_f[h]), right)
            down["g"] = g if h == 2 else down["g"] + g

        def filler(h):
            if h == 2:
                loads[5].wait()
                loads[6].wait()
            if h <= 5:
                dense((h - 2) // 2, (h - 2) % 2 * 2)
                dense((h - 2) // 2, (h - 2) % 2 * 2 + 1)
            if h == 6:
                loads[4].wait()
                arrived(t_k.at[1, 0], rk_sem.at[1, 0])
                arrived(t_k.at[1, 1], rk_sem.at[1, 1])
                side_terms(t_k[1, 0], t_k[1, 1])
                compose(2)
            if h == 7:
                compose(3)
                compose(4)
            if h == 8:
                compose(5)

        arrived(r_f.at[1], rf_sem.at[1])
        arrived(r_t.at[1], rt_sem.at[1], "wait_t1")
        current = lifted + r_t[1].astype(F32)
        for h in range(2, TOP + 1):
            cond, near, far = route(h)
            s_f[h] = current.astype(BF)
            if h == TOP:
                def go():
                    for k, (p, c) in enumerate(((far, 1), (near, 1), (far, 0), (near, 0))):
                        send_f(h, p, c, k).start()
                when(cond, go)
                break
            when(cond, lambda: send_f(h, near if far is None else far, 1, 0).start())
            arrived(t_pq.at[h - 1], rpq_sem.at[h - 1], f"wait_pq{h - 1}")
            term = mm(mm_t0(t_pq[h - 1, 0], current), t_pq[h - 1, 1])
            s_t[h] = term.astype(BF)

            def go():
                if far is not None:
                    send_t(h, far, 2).start()
                send_t(h, near, 1).start()
                if far is not None:
                    send_f(h, near, 1, 3).start()
            when(cond, go)
            with jax.named_scope(f"fill{h}"):
                filler(h)
            arrived(r_t.at[h], rt_sem.at[h], f"wait_t{h}")
            current = term + r_t[h].astype(F32)
            arrived(r_f.at[h], rf_sem.at[h], f"wait_f{h}")
        compose(6)
        compose(7)
        compose(8)
        left, right = compose(9)
        s_fin[0] = left
        s_fin[1] = right
        s_g[...] = down["g"]
        fin = [
            remote(s_fin.at[0], r_fin.at[0], fs_sem.at[0], fr_sem.at[0], row, me_c - 1),
            remote(s_fin.at[1], r_fin.at[1], fs_sem.at[1], fr_sem.at[1], row, me_c - 1),
            remote(s_g, r_g, fs_sem.at[2], fr_sem.at[2], row, me_c - 1),
        ]
        for c in fin:
            c.start()
        finish(down["g"], left, right)
        send.wait_send()
        for c in fin + hand_over(low, low_sem):
            c.wait_send()
        for h in range(2, TOP + 1):
            cond, near, far = route(h)

            def drain():
                if h == TOP:
                    for k, (p, c) in enumerate(((far, 1), (near, 1), (far, 0), (near, 0))):
                        send_f(h, p, c, k).wait_send()
                    return
                send_f(h, near if far is None else far, 1, 0).wait_send()
                if far is not None:
                    send_t(h, far, 2).wait_send()
                send_t(h, near, 1).wait_send()
                if far is not None:
                    send_f(h, near, 1, 3).wait_send()
            when(cond, drain)

    @pl.when(core == 0)
    def _():
        peer = y * 2 + 1
        mine = [
            remote(s_t.at[1], r_t.at[1], xs_sem.at[1, 0], rt_sem.at[1], row, peer),
            remote(s_f.at[1], r_f.at[1], xs_sem.at[1, 1], rf_sem.at[1], row, peer),
            remote(vasc.at[3], t_pq.at[1], xs_sem.at[2, 0], rpq_sem.at[1], row, peer),
        ]
        for c in mine:
            c.start()
        loads[2].wait()
        loads[3].wait()
        more = [
            remote(vdesc.at[3], t_sw.at[1], xs_sem.at[2, 1], rsw_sem.at[1], row, peer),
            remote(vcp.at[1, 1], t_k.at[1, 0], xs_sem.at[3, 0], rk_sem.at[1, 0], row, peer),
            remote(vcp.at[1, 2], t_k.at[1, 1], xs_sem.at[3, 1], rk_sem.at[1, 1], row, peer),
        ]
        for c in more:
            c.start()
        mine += more

        def low_copies(h):
            size = 2 ** (h - 1)
            base = y - y % size
            for i in range(size):
                yield table_copies(low, h, row, (base + i) * 2 + 1, i // (size // 2), i)

        @pl.when(y != 7)
        def _():
            arrived(low.at[pl.ds(0, 2)], low_sem.at[0], "wait_low")
            for h in (2, 3, 4):
                @pl.when(y % 2 ** (h - 1) == 2 ** (h - 2) - 1)
                def _():
                    for c in low_copies(h):
                        c[0]()[0].start()
            arrived(low.at[pl.ds(2, 2)], low_sem.at[1])
            arrived(low.at[pl.ds(4, 4)], low_sem.at[2])
            for h in (2, 3, 4):
                @pl.when(y % 2 ** (h - 1) == 2 ** (h - 2) - 1)
                def _():
                    for k in (2, 1):
                        for c in low_copies(h):
                            for d in c[k]():
                                d.start()

        parts = (pl.ds(0, 2), pl.ds(2, 2), pl.ds(4, 4))

        def ring_copy(k, j):
            return remote(
                top.at[parts[k]], top.at[parts[k]], y_sem.at[k, j], top_sem.at[k], row, j * 2
            )

        def owns(h):
            return row % 2 ** (h - 4) == 2 ** (h - 5) - 1

        def plane_copy(h, i):
            size = 2 ** (h - 4)
            return table_copies(top, h, row - row % size + i, peer, i // (size // 2), i)

        def upper(k):
            heights = (5, 6, 7, 8, 9) if k == 2 else (5, 6, 7)
            at_top = row % 32 != 31 if k == 2 else row % 8 != 7

            @pl.when(at_top)
            def _():
                arrived(top.at[parts[k]], top_sem.at[k], f"wait_top{k}")

                @pl.when(y == 7)
                def _():
                    for j in (3, 4, 2, 5, 1, 0, 6):
                        ring_copy(k, j).start()

                for h in heights:
                    @pl.when(owns(h))
                    def _():
                        def body(i, carry):
                            for d in plane_copy(h, i)[k]():
                                d.start()
                            return carry
                        lax.fori_loop(0, 2 ** (h - 4), body, 0)

        def local_work():
            loads[5].wait()
            loads[6].wait()
            for i in range(2):
                for r in range(4):
                    dense(i, r)
            loads[4].wait()
            arrived(r_f.at[1], rf_sem.at[1])
            side_terms(vcp[1, 0], vcp[1, 3])

        @pl.when(y == 7)
        def _():
            upper(0)

        with jax.named_scope("local"):
            local_work()

        @pl.when(y != 7)
        def _():
            upper(0)

        upper(2)
        upper(1)

        arrived(r_fin.at[0], fr_sem.at[0])
        arrived(r_fin.at[1], fr_sem.at[1])
        arrived(r_g, fr_sem.at[2], "wait_g")
        finish(r_g[...], r_fin[0], r_fin[1])

        for c in mine:
            c.wait_send()

        @pl.when(y != 7)
        def _():
            for h in (2, 3, 4):
                @pl.when(y % 2 ** (h - 1) == 2 ** (h - 2) - 1)
                def _():
                    for c in low_copies(h):
                        for k in range(3):
                            for d in c[k]():
                                d.wait_send()

        for k in range(3):
            heights = (5, 6, 7, 8, 9) if k == 2 else (5, 6, 7)
            at_top = row % 32 != 31 if k == 2 else row % 8 != 7

            @pl.when(at_top)
            def _():
                @pl.when(y == 7)
                def _():
                    for j in range(7):
                        ring_copy(k, j).wait_send()

                for h in heights:
                    @pl.when(owns(h))
                    def _():
                        def body(i, carry):
                            for d in plane_copy(h, i)[k]():
                                d.wait_send()
                            return carry
                        lax.fori_loop(0, 2 ** (h - 4), body, 0)

            @pl.when(jnp.logical_not(at_top))
            def _():
                @pl.when(y == 7)
                def _():
                    arrived(top.at[parts[k]], top_sem.at[k])


def shards(dense_a, dense_b, inner, outer, ascent, descent, couplings):
    any_spec = pl.BlockSpec(memory_space=pl.ANY)
    dma = pltpu.SemaphoreType.DMA
    tile = (128, 128)
    return pl.pallas_call(
        kernel,
        out_shape=jax.ShapeDtypeStruct((2, 512, 512), BF),
        in_specs=[any_spec] * 7,
        out_specs=any_spec,
        scratch_shapes=[
            pltpu.VMEM((2, 512, 512), BF),
            pltpu.VMEM((2, 512, 512), BF),
            pltpu.VMEM((2, 2, 512, 128), BF),
            pltpu.VMEM((2, 2, 512, 128), BF),
            pltpu.VMEM((4, 2, *tile), BF),
            pltpu.VMEM((4, 2, *tile), BF),
            pltpu.VMEM((2, 4, *tile), BF),
            pltpu.VMEM((2, 512, 512), F32),
            pltpu.VMEM((2, 512, 512), BF),
            pltpu.VMEM((2, 512, 128), BF),
            pltpu.VMEM((2, 512, 128), BF),
            pltpu.VMEM((10, *tile), BF),
            pltpu.VMEM((10, *tile), BF),
            pltpu.VMEM((10, *tile), BF),
            pltpu.VMEM((10, *tile), BF),
            pltpu.VMEM((8, 2, *tile), BF),
            pltpu.VMEM((8, 2, *tile), BF),
            pltpu.VMEM((10, 2, *tile), BF),
            pltpu.VMEM((8, *tile), BF),
            pltpu.VMEM((8, *tile), BF),
            pltpu.VMEM((2, *tile), F32),
            pltpu.VMEM((2, *tile), F32),
            pltpu.VMEM(tile, F32),
            pltpu.VMEM(tile, F32),
            dma((7,)),
            dma((4,)),
            dma((10, 4)),
            dma((10,)),
            dma((10,)),
            dma((8,)),
            dma((8,)),
            dma((10, 2)),
            dma((3,)),
            dma((3,)),
            dma((3,)),
            dma((3, 7)),
            dma((4, 32)),
            dma((3,)),
            dma((3,)),
        ],
        compiler_params=pltpu.CompilerParams(collective_id=0, has_side_effects=True),
        name="tree",
    )(dense_a, dense_b, inner, outer, ascent, descent, couplings)


def solution(mesh):
    placed = (
        P(("row", "col"), None, None),
        P(("row", "col"), None, None),
        P(("row", "col"), None, None, None),
        P(("row", "col"), None, None, None),
        P(("row", "col"), None, None, None, None),
        P(("row", "col"), None, None, None, None),
        P(("row", "col"), None, None, None, None),
    )
    return jax.shard_map(
        shards, mesh=mesh, in_specs=placed, out_specs=P(("row", "col"), None, None), check_vma=False
    )
```

```python
import jax
import jax.numpy as jnp
from jax import lax
from jax.experimental import pallas as pl
from jax.experimental.pallas import tpu as pltpu
from jax.sharding import PartitionSpec as P

MESH_ID = pl.DeviceIdType.MESH
BF = jnp.bfloat16
F32 = jnp.float32
N_X = 4
N_Y = 8
N_Z = 8
TOP = 9


def flip1(p):
    return p + 1 - 2 * (p % 2)


def flip3(p):
    return p - p % 4 + 3 - p % 4


def halves(v):
    if v.dtype == BF:
        return (v,)
    high = v.astype(BF)
    return high, (v - high.astype(F32)).astype(BF)


def product(a, b, ca, cb):
    a, b = halves(a), halves(b)
    terms = [(i, j) for i in range(len(a)) for j in range(len(b)) if i + j < 2]
    if len(terms) == 1:
        left, right = a[0], b[0]
    else:
        left = jnp.concatenate([a[i] for i, _ in terms], ca)
        right = jnp.concatenate([b[j] for _, j in terms], cb)
    return lax.dot_general(left, right, (((ca,), (cb,)), ((), ())), preferred_element_type=F32)


def mm(a, b):
    return product(a, b, 1, 0)


def mm_t0(a, b):
    return product(a, b, 0, 0)


def mm_t1(a, b):
    return product(a, b, 1, 1)


def kernel(
    da, db, ib, ob, asc, desc, cp, out,
    va, vb, vib, vob, vasc, vdesc, vcp,
    acc, obuf, us, vw, s_f, s_t, r_f, r_t,
    t_pq, t_sw, t_k, low, top, s_fin, r_fin,
    ld_sem, st_sem, xs_sem, rf_sem, rt_sem, rpq_sem, rsw_sem, rk_sem,
    hs_sem, low_sem, top_sem, y_sem, tab_sem, lows_sem, own_sem, fs_sem, fr_sem, go_sem,
):
    row = lax.axis_index("row")
    col = lax.axis_index("col")
    z, x = row // N_X, row % N_X
    y, core = col // 2, col % 2

    def position(h):
        return y if h <= 4 else x if h <= 6 else z

    def route(h):
        p = position(h)
        if h in (2, 5, 7):
            return None, flip1(p), None
        if h == 6:
            return None, 3 - p, None
        middle = ((p + 1) // 2) % 2
        if h in (3, 8):
            near = flip3(p)
            return middle == 1, near, flip1(near)
        near = 7 - p
        return middle == 0, near, flip1(near)

    def sender(h, p):
        if h in (2, 5, 7):
            return flip1(p)
        if h == 6:
            return 3 - p
        middle = ((p + 1) // 2) % 2
        if h in (3, 8):
            return jnp.where(middle == 1, flip3(p), flip1(flip3(p)))
        return jnp.where(middle == 0, 7 - p, flip1(7 - p))

    def place(h, p, c):
        if h <= 4:
            return row, p * 2 + c
        if h <= 6:
            return z * N_X + p, y * 2 + c
        return p * N_X + x, y * 2 + c

    loads = []
    pairs = ((ib, vib), (asc.at[0], vasc), (desc.at[0], vdesc), (cp.at[0], vcp), (ob, vob), (da, va), (db, vb))
    for i, (src, dst) in enumerate(pairs):
        c = pltpu.make_async_copy(src, dst, ld_sem.at[i])
        c.start()
        loads.append(c)

    barrier = pltpu.get_barrier_semaphore()

    def greet(r, c):
        pl.semaphore_signal(barrier, inc=1, device_id=(r, c), device_id_type=MESH_ID)

    middle_y, middle_z = ((y + 1) // 2) % 2, ((z + 1) // 2) % 2
    low_size = jnp.where(y % 2 == 0, 2, jnp.where(y % 4 == 1, 4, 8))
    top_size = jnp.where(x % 2 == 0, 2, jnp.where(x == 1, 4, jnp.where(z % 2 == 0, 8, jnp.where(z % 4 == 1, 16, 32))))
    top_size = jnp.where(row == N_X * N_Z - 1, 0, top_size)

    @pl.when(core == 0)
    def _():
        greet(row, col + 1)
        greet(sender(TOP, z) * N_X + x, y * 2 + 1)

        @pl.when(y != 7)
        def _():
            greet(row, 14)

    @pl.when(core == 1)
    def _():
        greet(row, col - 1)
        for h in (2, 3, 4):
            greet(row, (y - y % 2 ** (h - 1) + 2 ** (h - 2) - 1) * 2)
        for h in range(2, TOP + 1):
            greet(*place(h, sender(h, position(h)), 1))
        for h in range(5, TOP + 1):
            greet(row - row % 2 ** (h - 4) + 2 ** (h - 5) - 1, y * 2)

    receivers = jnp.where(
        core == 0,
        1 + jnp.where(y == 7, 7, low_size) + top_size,
        5 + 2 * middle_y + 2 * (1 - middle_y) + 2 * middle_z + 4 * (1 - middle_z),
    )

    with jax.named_scope("load"):
        loads[0].wait()
        loads[1].wait()
    leaf = [mm_t0(vib[i, 0], vib[i, 1]) for i in range(2)]
    term = [mm(mm_t0(vasc[i, 0], leaf[i]), vasc[i, 1]) for i in range(2)]
    node = term[0] + term[1]
    lifted = mm(mm_t0(vasc[2, 0], node), vasc[2, 1])
    s_f[1] = node.astype(BF)
    s_t[1] = lifted.astype(BF)

    with jax.named_scope("entry"):
        pl.semaphore_wait(barrier, receivers)

    def remote(src, dst, ssem, rsem, r, c):
        return pltpu.make_async_remote_copy(
            src_ref=src, dst_ref=dst, send_sem=ssem, recv_sem=rsem,
            device_id=(r, c), device_id_type=MESH_ID,
        )

    def arrived(dst, sem, name="wait"):
        with jax.named_scope(name):
            remote(dst, dst, xs_sem.at[0], sem, row, col).wait_recv()

    def sent(src, sem):
        remote(src, src, sem, rf_sem.at[0], row, col).wait_send()

    def dense(i, r):
        rows = pl.ds(r * 128, 128)
        acc[i, rows, :] = jnp.dot(va[i, rows, :], vb[i], preferred_element_type=F32)

    def side_terms(i, kl1, kr1):
        near_node = mm(mm(kl1, r_f[1]), kr1)
        if True:
            kl, kr = (vcp[0, 0], vcp[0, 3]) if i == 0 else (vcp[0, 1], vcp[0, 2])
            g = mm(mm(kl, leaf[1 - i]), kr)
            g = g + mm_t1(mm(vdesc[i, 0], near_node), vdesc[i, 1])
            us[i] = mm(vob[i, 0], mm(vdesc[i, 0], vdesc[2, 0])).astype(BF)
            vw[i] = mm(vob[i, 1], mm(vdesc[i, 1], vdesc[2, 1])).astype(BF)
            acc[i] += mm_t1(mm(vob[i, 0], g.astype(BF)).astype(BF), vob[i, 1])

    def finish(g, left, right):
        arrived(r_f.at[TOP], rf_sem.at[TOP], "wait_f9")
        g = (g + mm(mm(left, r_f[TOP]), right)).astype(BF)
        for i in range(2):
            spread = mm(us[i], g).astype(BF)
            for r in range(2):
                rows = pl.ds(r * 256, 256)
                block = acc[i, rows, :] + mm_t1(spread[r * 256:(r + 1) * 256], vw[i])
                obuf[i, rows, :] = block.astype(BF)
                c = pltpu.make_async_copy(obuf.at[i, rows], out.at[i, rows], st_sem)
                c.start()
        with jax.named_scope("stores"):
            pltpu.make_async_copy(obuf, out, st_sem).wait()

    def when(cond, f):
        if cond is None:
            f()
        else:
            pl.when(cond)(f)

    def send_f(h, p, c):
        r, cc = place(h, p, c)
        return remote(s_f.at[h], r_f.at[h], xs_sem.at[h], rf_sem.at[h], r, cc)

    def send_t(h, p):
        r, cc = place(h, p, 1)
        return remote(s_t.at[h], r_t.at[h], xs_sem.at[h], rt_sem.at[h], r, cc)

    def table_copies(src, sem, h, r, c, side):
        return (
            lambda: (remote(src.at[pl.ds(0, 2)], t_pq.at[h], sem.at[0], rpq_sem.at[h], r, c),),
            lambda: (remote(src.at[pl.ds(2, 2)], t_sw.at[h], sem.at[1], rsw_sem.at[h], r, c),),
            lambda: (
                remote(src.at[4 + side], t_k.at[h, 0], sem.at[2], rk_sem.at[h], r, c),
                remote(src.at[7 - side], t_k.at[h, 1], sem.at[2], rk_sem.at[h], r, c),
            ),
        )

    @pl.when(core == 1)
    def _():
        me_c = y * 2 + 1
        send = remote(s_f.at[1], r_f.at[1], xs_sem.at[1], rf_sem.at[1], row, me_c - 1)
        send.start()
        loads[2].wait()
        loads[3].wait()

        def hand_over(dst, sems):
            return [
                remote(vasc.at[3], dst.at[pl.ds(0, 2)], hs_sem.at[0], sems.at[0], row, me_c - 1),
                remote(vdesc.at[3], dst.at[pl.ds(2, 2)], hs_sem.at[0], sems.at[1], row, me_c - 1),
                remote(vcp.at[1], dst.at[pl.ds(4, 4)], hs_sem.at[0], sems.at[2], row, me_c - 1),
            ]

        @pl.when(y == 7)
        def _():
            for c in hand_over(top, top_sem):
                c.start()

        @pl.when(y != 7)
        def _():
            for c in hand_over(low, low_sem):
                c.start()

        down = {}

        def compose(h):
            arrived(t_k.at[h], rk_sem.at[h], f"wait_k{h}")
            left, right = t_k[h, 0], t_k[h, 1]
            if h >= 3:
                arrived(t_sw.at[h - 2], rsw_sem.at[h - 2], f"wait_sw{h - 2}")
                s, w = t_sw[h - 2, 0], t_sw[h - 2, 1]
                if h == 3:
                    down["s"], down["w"] = s, w.T
                else:
                    down["s"] = mm(down["s"], s)
                    down["w"] = mm_t0(w, down["w"])
                left = mm(down["s"], left)
                right = mm(right, down["w"])
            if h == TOP:
                return left, right
            g = mm(mm(left, r_f[h]), right)
            down["g"] = g if h == 2 else down["g"] + g

        def filler(h):
            if h == 2:
                loads[5].wait()
                loads[6].wait()
                for r in range(4):
                    dense(0, r)
            if h == 3:
                for r in range(4):
                    dense(1, r)
                arrived(t_k.at[1], rk_sem.at[1])
                loads[4].wait()
                side_terms(0, t_k[1, 0], t_k[1, 1])
            if h == 4:
                side_terms(1, t_k[1, 0], t_k[1, 1])
            if h == 7:
                compose(2)
                compose(3)
            if h == 8:
                compose(4)
                compose(5)
                compose(6)

        arrived(r_f.at[1], rf_sem.at[1])
        arrived(r_t.at[1], rt_sem.at[1], "wait_t1")
        current = lifted + r_t[1].astype(F32)
        for h in range(2, TOP + 1):
            cond, near, far = route(h)
            s_f[h] = current.astype(BF)
            if h == TOP:
                def go():
                    for p, c in ((far, 1), (near, 1), (far, 0), (near, 0)):
                        send_f(h, p, c).start()
                when(cond, go)
                break
            when(cond, lambda: send_f(h, near if far is None else far, 1).start())
            arrived(t_pq.at[h - 1], rpq_sem.at[h - 1], f"wait_pq{h - 1}")
            term = mm(mm_t0(t_pq[h - 1, 0], current), t_pq[h - 1, 1])
            s_t[h] = term.astype(BF)

            def go():
                if far is not None:
                    send_t(h, far).start()
                send_t(h, near).start()
                if far is not None:
                    send_f(h, near, 1).start()
            when(cond, go)
            with jax.named_scope(f"fill{h}"):
                filler(h)
            arrived(r_t.at[h], rt_sem.at[h], f"wait_t{h}")
            current = term + r_t[h].astype(F32)
            if h == 4:
                pl.semaphore_signal(go_sem, inc=1, device_id=(row, me_c - 1), device_id_type=MESH_ID)
            arrived(r_f.at[h], rf_sem.at[h], f"wait_f{h}")
        compose(7)
        compose(8)
        left, right = compose(9)
        s_fin[0] = left
        s_fin[1] = right
        s_fin[2] = down["g"]
        fin = remote(s_fin, r_fin, fs_sem, fr_sem, row, me_c - 1)
        fin.start()
        finish(down["g"], left, right)
        send.wait_send()
        fin.wait_send()
        sent(low, hs_sem.at[0])
        for h in range(2, TOP + 1):
            cond, near, far = route(h)
            count = 2 if far is None else 4
            when(cond, lambda: sent(s_f.at[pl.ds(0, count)], xs_sem.at[h]))

    @pl.when(core == 0)
    def _():
        peer = y * 2 + 1
        mine = [
            remote(s_t.at[1], r_t.at[1], own_sem.at[0], rt_sem.at[1], row, peer),
            remote(s_f.at[1], r_f.at[1], own_sem.at[1], rf_sem.at[1], row, peer),
            remote(vasc.at[3], t_pq.at[1], own_sem.at[2], rpq_sem.at[1], row, peer),
        ]
        for c in mine:
            c.start()
        loads[2].wait()
        loads[3].wait()
        more = [
            remote(vdesc.at[3], t_sw.at[1], own_sem.at[3], rsw_sem.at[1], row, peer),
            remote(vcp.at[1, 1], t_k.at[1, 0], own_sem.at[4], rk_sem.at[1], row, peer),
            remote(vcp.at[1, 2], t_k.at[1, 1], own_sem.at[5], rk_sem.at[1], row, peer),
        ]
        for c in more:
            c.start()
        mine += more

        def low_copies(h):
            size = 2 ** (h - 1)
            base = y - y % size
            for i in range(size):
                yield table_copies(low, lows_sem, h, row, (base + i) * 2 + 1, i // (size // 2))

        @pl.when(y != 7)
        def _():
            arrived(low.at[pl.ds(0, 2)], low_sem.at[0], "wait_low")
            for h in (2, 3, 4):
                @pl.when(y % 2 ** (h - 1) == 2 ** (h - 2) - 1)
                def _():
                    for c in low_copies(h):
                        c[0]()[0].start()

        def low_rest():
            arrived(low.at[pl.ds(2, 2)], low_sem.at[1])
            arrived(low.at[pl.ds(4, 4)], low_sem.at[2])
            for h in (2, 3, 4):
                @pl.when(y % 2 ** (h - 1) == 2 ** (h - 2) - 1)
                def _():
                    for k in (2, 1):
                        for c in low_copies(h):
                            for d in c[k]():
                                d.start()

        parts = (pl.ds(0, 2), pl.ds(2, 2), pl.ds(4, 4))

        def ring_copy(k, j):
            return remote(
                top.at[parts[k]], top.at[parts[k]], y_sem.at[k], top_sem.at[k], row, j * 2
            )

        def owns(h):
            return row % 2 ** (h - 4) == 2 ** (h - 5) - 1

        def plane_copy(h, i):
            size = 2 ** (h - 4)
            return table_copies(top, tab_sem, h, row - row % size + i, peer, i // (size // 2))

        def upper(k, heights):
            here = (row % 8 != 7) if heights[0] == 5 else (row % 8 == 7) & (row != 31)

            @pl.when(here)
            def _():
                arrived(top.at[parts[k]], top_sem.at[k], f"wait_top{k}")

                @pl.when(y == 7)
                def _():
                    for j in (3, 4, 2, 5, 1, 0, 6):
                        ring_copy(k, j).start()

                for h in heights:
                    @pl.when(owns(h))
                    def _():
                        def body(i, carry):
                            for d in plane_copy(h, i)[k]():
                                d.start()
                            return carry
                        lax.fori_loop(0, 2 ** (h - 4), body, 0)

        def first_tables():
            upper(0, (5, 6, 7))
            upper(2, (8, 9))

        def local_work():
            loads[5].wait()
            loads[6].wait()
            for i in range(2):
                for r in range(4):
                    dense(i, r)
            loads[4].wait()
            arrived(r_f.at[1], rf_sem.at[1])
            for i in range(2):
                side_terms(i, vcp[1, 0], vcp[1, 3])

        @pl.when(y == 7)
        def _():
            first_tables()

        with jax.named_scope("local"):
            local_work()

        @pl.when(y != 7)
        def _():
            first_tables()

        with jax.named_scope("go"):
            pl.semaphore_wait(go_sem, 1)
        upper(2, (5, 6, 7))
        pl.when(y != 7)(low_rest)
        upper(1, (5, 6, 7))

        arrived(r_fin, fr_sem, "wait_fin")
        finish(r_fin[2], r_fin[0], r_fin[1])

        for c in mine:
            c.wait_send()

        @pl.when(y != 7)
        def _():
            for h in (2, 3, 4):
                @pl.when(y % 2 ** (h - 1) == 2 ** (h - 2) - 1)
                def _():
                    for k in range(3):
                        sent(acc.at[0, pl.ds(0, 32 * 2 ** (h - 1))], lows_sem.at[k])

        def drained(k, heights):
            here = (row % 8 != 7) if heights[0] == 5 else (row % 8 == 7) & (row != 31)

            @pl.when(here)
            def _():
                @pl.when(y == 7)
                def _():
                    sent(acc.at[0, pl.ds(0, 32 * 7 * (2 if k == 2 else 1))], y_sem.at[k])

                for h in heights:
                    @pl.when(owns(h))
                    def _():
                        if h == 9:
                            sent(acc, tab_sem.at[k])
                        else:
                            sent(acc.at[0, pl.ds(0, 32 * 2 ** (h - 4))], tab_sem.at[k])

        drained(0, (5, 6, 7))
        drained(1, (5, 6, 7))
        drained(2, (5, 6, 7))
        drained(2, (8, 9))

        @pl.when((y == 7) & (row % 8 == 7))
        def _():
            arrived(top.at[parts[0]], top_sem.at[0])
            arrived(top.at[parts[1]], top_sem.at[1])

        @pl.when((y == 7) & (row == 31))
        def _():
            arrived(top.at[parts[2]], top_sem.at[2])


def shards(dense_a, dense_b, inner, outer, ascent, descent, couplings):
    any_spec = pl.BlockSpec(memory_space=pl.ANY)
    dma = pltpu.SemaphoreType.DMA
    tile = (128, 128)
    return pl.pallas_call(
        kernel,
        out_shape=jax.ShapeDtypeStruct((2, 512, 512), BF),
        in_specs=[any_spec] * 7,
        out_specs=any_spec,
        scratch_shapes=[
            pltpu.VMEM((2, 512, 512), BF),
            pltpu.VMEM((2, 512, 512), BF),
            pltpu.VMEM((2, 2, 512, 128), BF),
            pltpu.VMEM((2, 2, 512, 128), BF),
            pltpu.VMEM((4, 2, *tile), BF),
            pltpu.VMEM((4, 2, *tile), BF),
            pltpu.VMEM((2, 4, *tile), BF),
            pltpu.VMEM((2, 512, 512), F32),
            pltpu.VMEM((2, 512, 512), BF),
            pltpu.VMEM((2, 512, 128), BF),
            pltpu.VMEM((2, 512, 128), BF),
            pltpu.VMEM((10, *tile), BF),
            pltpu.VMEM((10, *tile), BF),
            pltpu.VMEM((10, *tile), BF),
            pltpu.VMEM((10, *tile), BF),
            pltpu.VMEM((8, 2, *tile), BF),
            pltpu.VMEM((8, 2, *tile), BF),
            pltpu.VMEM((10, 2, *tile), BF),
            pltpu.VMEM((8, *tile), BF),
            pltpu.VMEM((8, *tile), BF),
            pltpu.VMEM((3, *tile), F32),
            pltpu.VMEM((3, *tile), F32),
            dma((7,)),
            dma,
            dma((10,)),
            dma((10,)),
            dma((10,)),
            dma((8,)),
            dma((8,)),
            dma((10,)),
            dma((1,)),
            dma((3,)),
            dma((3,)),
            dma((3,)),
            dma((3,)),
            dma((3,)),
            dma((6,)),
            dma,
            dma,
            pltpu.SemaphoreType.REGULAR,
        ],
        compiler_params=pltpu.CompilerParams(collective_id=0, has_side_effects=True),
        name="tree",
    )(dense_a, dense_b, inner, outer, ascent, descent, couplings)


def solution(mesh):
    placed = (
        P(("row", "col"), None, None),
        P(("row", "col"), None, None),
        P(("row", "col"), None, None, None),
        P(("row", "col"), None, None, None),
        P(("row", "col"), None, None, None, None),
        P(("row", "col"), None, None, None, None),
        P(("row", "col"), None, None, None, None),
    )
    return jax.shard_map(
        shards, mesh=mesh, in_specs=placed, out_specs=P(("row", "col"), None, None), check_vma=False
    )
```

```python
import jax
import jax.numpy as jnp
from jax import lax
from jax.experimental import pallas as pl
from jax.experimental.pallas import tpu as pltpu
from jax.sharding import PartitionSpec as P

MESH_ID = pl.DeviceIdType.MESH
BF = jnp.bfloat16
F32 = jnp.float32
N_X = 4
N_Y = 8
N_Z = 8
GO = 3
TOP = 9


def flip1(p):
    return p + 1 - 2 * (p % 2)


def flip3(p):
    return p - p % 4 + 3 - p % 4


def halves(v):
    if v.dtype == BF:
        return (v,)
    high = v.astype(BF)
    return high, (v - high.astype(F32)).astype(BF)


def product(a, b, ca, cb):
    a, b = halves(a), halves(b)
    terms = [(i, j) for i in range(len(a)) for j in range(len(b)) if i + j < 2]
    if len(terms) == 1:
        left, right = a[0], b[0]
    else:
        left = jnp.concatenate([a[i] for i, _ in terms], ca)
        right = jnp.concatenate([b[j] for _, j in terms], cb)
    return lax.dot_general(left, right, (((ca,), (cb,)), ((), ())), preferred_element_type=F32)


def mm(a, b):
    return product(a, b, 1, 0)


def mm_t0(a, b):
    return product(a, b, 0, 0)


def mm_t1(a, b):
    return product(a, b, 1, 1)


def kernel(
    da, db, ib, ob, asc, desc, cp, out,
    va, vb, vib, vob, vasc, vdesc, vcp,
    acc, obuf, us, vw, s_f, s_t, r_f, r_t,
    t_pq, t_sw, t_k, low, top, mid, s_fin, r_fin,
    ld_sem, st_sem, xs_sem, rf_sem, rt_sem, rpq_sem, rsw_sem, rk_sem,
    hs_sem, low_sem, top_sem, mid_sem, y_sem, tab_sem, lows_sem, own_sem, fs_sem, fr_sem, go_sem, rdy_sem, mrdy_sem, hd_sem,
):
    row = lax.axis_index("row")
    col = lax.axis_index("col")
    z, x = row // N_X, row % N_X
    y, core = col // 2, col % 2

    def position(h):
        return y if h <= 4 else x if h <= 6 else z

    def route(h):
        p = position(h)
        if h in (2, 5, 7):
            return None, flip1(p), None
        if h == 6:
            return None, 3 - p, None
        middle = ((p + 1) // 2) % 2
        if h in (3, 8):
            near = flip3(p)
            return middle == 1, near, flip1(near)
        near = 7 - p
        return middle == 0, near, flip1(near)

    def sender(h, p):
        if h in (2, 5, 7):
            return flip1(p)
        if h == 6:
            return 3 - p
        middle = ((p + 1) // 2) % 2
        if h in (3, 8):
            return jnp.where(middle == 1, flip3(p), flip1(flip3(p)))
        return jnp.where(middle == 0, 7 - p, flip1(7 - p))

    def place(h, p, c):
        if h <= 4:
            return row, p * 2 + c
        if h <= 6:
            return z * N_X + p, y * 2 + c
        return p * N_X + x, y * 2 + c

    def keeper(h):
        size = 2 ** (h - 6)
        return z - z % size + size // 2 - 1

    loads = []
    pairs = ((ib, vib), (asc.at[0], vasc), (desc.at[0], vdesc), (cp.at[0], vcp), (ob, vob), (da, va), (db, vb))
    for i, (src, dst) in enumerate(pairs):
        c = pltpu.make_async_copy(src, dst, ld_sem.at[i])
        c.start()
        loads.append(c)

    barrier = pltpu.get_barrier_semaphore()

    def greet(r, c):
        pl.semaphore_signal(barrier, inc=1, device_id=(r, c), device_id_type=MESH_ID)

    middle_y, middle_z = ((y + 1) // 2) % 2, ((z + 1) // 2) % 2
    low_size = jnp.where(y % 2 == 0, 2, jnp.where(y % 4 == 1, 4, 8))
    below = jnp.where(z % 2 == 0, 1, jnp.where(z % 4 == 1, 3, jnp.where(z == 3, 3, 0)))
    upper_half = z // 4
    top_size = jnp.where(x % 2 == 0, 2, jnp.where(x == 1, 4, 12 + below))
    relay = jnp.where((y % 2 == 0) & (y != 4), 1, 0)

    @pl.when(core == 0)
    def _():
        greet(row, col + 1)
        pl.when(upper_half == 0)(lambda: greet(sender(TOP, z) * N_X + x, y * 2 + 1))

        for h in (7, 8, 9):
            @pl.when((x == 3) & (z != keeper(h)) & ((h < 9) | (upper_half == 0)))
            def _():
                greet(keeper(h) * N_X + 3, y * 2)

        @pl.when(row == 15)
        def _():
            for i in range(4, 8):
                greet(i * N_X + 3, y * 2)

        @pl.when(y != 7)
        def _():
            greet(row, jnp.where(y % 2 == 0, 7, jnp.where(y == 5, 6, y - 1)) * 2)

    @pl.when(core == 1)
    def _():
        greet(row, col - 1)
        for h in (2, 3, 4):
            greet(row, (y - y % 2 ** (h - 1) + 2 ** (h - 2) - 1) * 2)
        for h in range(2, TOP):
            greet(*place(h, sender(h, position(h)), 1))
        pl.when(upper_half == 0)(lambda: greet(*place(TOP, sender(TOP, z), 1)))

        @pl.when((upper_half == 0) & (middle_z == 0))
        def _():
            for c in (0, 1):
                greet(*place(TOP, 7 - z, c))
                greet(*place(TOP, flip1(7 - z), c))

        for holder in (x - x % 2, 1, 3, 3, 3):
            greet(z * N_X + holder, y * 2)

    receivers = jnp.where(
        core == 0,
        1 + jnp.where(y == 7, 4, low_size) + relay + top_size + upper_half * (1 + x // 3),
        5 + 2 + 2 * middle_z + upper_half * (4 * (1 - middle_z) + 1),
    )

    with jax.named_scope("load"):
        loads[0].wait()
        loads[1].wait()
    leaf = [mm_t0(vib[i, 0], vib[i, 1]) for i in range(2)]
    term = [mm(mm_t0(vasc[i, 0], leaf[i]), vasc[i, 1]) for i in range(2)]
    node = term[0] + term[1]
    lifted = mm(mm_t0(vasc[2, 0], node), vasc[2, 1])
    s_f[1] = node.astype(BF)
    s_t[1] = lifted.astype(BF)

    with jax.named_scope("entry"):
        pl.semaphore_wait(barrier, receivers)

    @pl.when(upper_half == 1)
    def _():
        pl.semaphore_signal(rdy_sem, inc=1, device_id=place(TOP, sender(TOP, z), 1), device_id_type=MESH_ID)

        @pl.when((core == 0) & (x == 3))
        def _():
            pl.semaphore_signal(mrdy_sem, inc=1, device_id=(15, y * 2), device_id_type=MESH_ID)

    def remote(src, dst, ssem, rsem, r, c):
        return pltpu.make_async_remote_copy(
            src_ref=src, dst_ref=dst, send_sem=ssem, recv_sem=rsem,
            device_id=(r, c), device_id_type=MESH_ID,
        )

    def arrived(dst, sem, name="wait"):
        with jax.named_scope(name):
            remote(dst, dst, xs_sem.at[0], sem, row, col).wait_recv()

    def sent(src, sem):
        remote(src, src, sem, rf_sem.at[0], row, col).wait_send()

    def dense(i, r):
        rows = pl.ds(r * 128, 128)
        acc[i, rows, :] = jnp.dot(va[i, rows, :], vb[i], preferred_element_type=F32)

    def side_terms(i, kl1, kr1):
        near_node = mm(mm(kl1, r_f[1]), kr1)
        if True:
            kl, kr = (vcp[0, 0], vcp[0, 3]) if i == 0 else (vcp[0, 1], vcp[0, 2])
            g = mm(mm(kl, leaf[1 - i]), kr)
            g = g + mm_t1(mm(vdesc[i, 0], near_node), vdesc[i, 1])
            us[i] = mm(vob[i, 0], mm(vdesc[i, 0], vdesc[2, 0])).astype(BF)
            vw[i] = mm(vob[i, 1], mm(vdesc[i, 1], vdesc[2, 1])).astype(BF)
            acc[i] += mm_t1(mm(vob[i, 0], g.astype(BF)).astype(BF), vob[i, 1])

    def finish(g, left, right):
        arrived(r_f.at[TOP], rf_sem.at[TOP], "wait_f9")
        g = (g + mm(mm(left, r_f[TOP]), right)).astype(BF)
        for i in range(2):
            spread = mm(us[i], g).astype(BF)
            for r in range(2):
                rows = pl.ds(r * 256, 256)
                block = acc[i, rows, :] + mm_t1(spread[r * 256:(r + 1) * 256], vw[i])
                obuf[i, rows, :] = block.astype(BF)
                c = pltpu.make_async_copy(obuf.at[i, rows], out.at[i, rows], st_sem)
                c.start()
        with jax.named_scope("stores"):
            pltpu.make_async_copy(obuf, out, st_sem).wait()

    def when(cond, f):
        if cond is None:
            f()
        else:
            pl.when(cond)(f)

    def send_f(h, p, c):
        r, cc = place(h, p, c)
        return remote(s_f.at[h], r_f.at[h], xs_sem.at[h], rf_sem.at[h], r, cc)

    def send_t(h, p):
        r, cc = place(h, p, 1)
        return remote(s_t.at[h], r_t.at[h], xs_sem.at[h], rt_sem.at[h], r, cc)

    def table_copies(src, sem, h, r, c, side):
        return (
            lambda: (remote(src.at[pl.ds(0, 2)], t_pq.at[h], sem.at[0], rpq_sem.at[h], r, c),),
            lambda: (remote(src.at[pl.ds(2, 2)], t_sw.at[h], sem.at[1], rsw_sem.at[h], r, c),),
            lambda: (
                remote(src.at[4 if side is None else 4 + side], t_k.at[h, 0], sem.at[2], rk_sem.at[h], r, c),
                remote(src.at[5 if side is None else 7 - side], t_k.at[h, 1], sem.at[2], rk_sem.at[h], r, c),
            ),
        )

    @pl.when(core == 1)
    def _():
        me_c = y * 2 + 1
        send = remote(s_f.at[1], r_f.at[1], xs_sem.at[1], rf_sem.at[1], row, me_c - 1)
        send.start()
        loads[2].wait()
        loads[3].wait()

        def hand_over(dst, sems):
            return [
                remote(vasc.at[3], dst.at[pl.ds(0, 2)], hs_sem.at[0], sems.at[0], row, me_c - 1),
                remote(vdesc.at[3], dst.at[pl.ds(2, 2)], hs_sem.at[0], sems.at[1], row, me_c - 1),
                remote(vcp.at[1], dst.at[pl.ds(4, 4)], hs_sem.at[0], sems.at[2], row, me_c - 1),
            ]

        @pl.when(y == 7)
        def _():
            for c in hand_over(top, top_sem):
                c.start()

        @pl.when(y != 7)
        def _():
            for c in hand_over(low, low_sem):
                c.start()

        ahead = remote(vasc.at[3], t_pq.at[2], hd_sem, rpq_sem.at[2], row, me_c + 2)
        pl.when(y % 2 == 0)(lambda: ahead.start())

        down = {}

        def compose(h):
            arrived(t_k.at[h], rk_sem.at[h], f"wait_k{h}")
            left, right = t_k[h, 0], t_k[h, 1]
            if h >= 3:
                arrived(t_sw.at[h - 2], rsw_sem.at[h - 2], f"wait_sw{h - 2}")
                s, w = t_sw[h - 2, 0], t_sw[h - 2, 1]
                if h == 3:
                    down["s"], down["w"] = s, w.T
                else:
                    down["s"] = mm(down["s"], s)
                    down["w"] = mm_t0(w, down["w"])
                left = mm(down["s"], left)
                right = mm(right, down["w"])
            if h == TOP:
                return left, right
            arrived(r_f.at[h], rf_sem.at[h], f"wait_f{h}")
            g = mm(mm(left, r_f[h]), right)
            down["g"] = g if h == 2 else down["g"] + g

        def filler(h):
            if h == 2:
                loads[5].wait()
                loads[6].wait()
                for r in range(4):
                    dense(0, r)
            if h == 3:
                for r in range(4):
                    dense(1, r)
                arrived(t_k.at[1], rk_sem.at[1])
                loads[4].wait()
                side_terms(0, t_k[1, 0], t_k[1, 1])
            if h == 4:
                side_terms(1, t_k[1, 0], t_k[1, 1])
            if h == 7:
                compose(2)
                compose(3)
            if h == 8:
                compose(4)

        arrived(r_f.at[1], rf_sem.at[1])
        arrived(r_t.at[1], rt_sem.at[1], "wait_t1")
        current = lifted + r_t[1].astype(F32)
        for h in range(2, TOP + 1):
            cond, near, far = route(h)
            s_f[h] = current.astype(BF)
            if h == TOP:
                def go():
                    pl.when(upper_half == 0)(lambda: pl.semaphore_wait(rdy_sem, 4))
                    for p, c in ((far, 1), (near, 1), (far, 0), (near, 0)):
                        send_f(h, p, c).start()
                when(cond, go)
                break
            arrived(t_pq.at[h - 1], rpq_sem.at[h - 1], f"wait_pq{h - 1}")
            term = mm(mm_t0(t_pq[h - 1, 0], current), t_pq[h - 1, 1])
            s_t[h] = term.astype(BF)

            def go():
                if far is not None:
                    send_t(h, far).start()
                send_t(h, near).start()
                if far is not None:
                    send_f(h, far, 1).start()
                send_f(h, near, 1).start()
            when(cond, go)
            with jax.named_scope(f"fill{h}"):
                filler(h)
            arrived(r_t.at[h], rt_sem.at[h], f"wait_t{h}")
            current = term + r_t[h].astype(F32)
            if h == GO:
                pl.semaphore_signal(go_sem, inc=1, device_id=(row, me_c - 1), device_id_type=MESH_ID)
        compose(5)
        compose(6)
        compose(7)
        compose(8)
        left, right = compose(9)
        s_fin[0] = left
        s_fin[1] = right
        s_fin[2] = down["g"]
        fin = remote(s_fin, r_fin, fs_sem, fr_sem, row, me_c - 1)
        fin.start()
        finish(down["g"], left, right)
        send.wait_send()
        pl.when(y % 2 == 0)(lambda: ahead.wait_send())
        fin.wait_send()
        sent(low, hs_sem.at[0])
        for h in range(2, TOP + 1):
            cond, near, far = route(h)
            count = 2 if far is None else 4
            when(cond, lambda: sent(s_f.at[pl.ds(0, count)], xs_sem.at[h]))

    @pl.when(core == 0)
    def _():
        peer = y * 2 + 1
        mine = [
            remote(s_t.at[1], r_t.at[1], own_sem.at[0], rt_sem.at[1], row, peer),
            remote(s_f.at[1], r_f.at[1], own_sem.at[1], rf_sem.at[1], row, peer),
            remote(vasc.at[3], t_pq.at[1], own_sem.at[2], rpq_sem.at[1], row, peer),
        ]
        for c in mine:
            c.start()
        loads[2].wait()
        loads[3].wait()
        more = [
            remote(vdesc.at[3], t_sw.at[1], own_sem.at[3], rsw_sem.at[1], row, peer),
            remote(vcp.at[1, 1], t_k.at[1, 0], own_sem.at[4], rk_sem.at[1], row, peer),
            remote(vcp.at[1, 2], t_k.at[1, 1], own_sem.at[5], rk_sem.at[1], row, peer),
        ]
        for c in more:
            c.start()
        mine += more

        def low_copies(h):
            size = 2 ** (h - 1)
            base = y - y % size
            for i in range(size):
                yield table_copies(low, lows_sem, h, row, (base + i) * 2 + 1, i // (size // 2))

        @pl.when(y != 7)
        def _():
            arrived(low.at[pl.ds(0, 2)], low_sem.at[0], "wait_low")
            for h in (2, 3, 4):
                @pl.when(y % 2 ** (h - 1) == 2 ** (h - 2) - 1)
                def _():
                    for c in list(low_copies(h))[:1 if h == 2 else None]:
                        c[0]()[0].start()

        def low_rest():
            arrived(low.at[pl.ds(2, 2)], low_sem.at[1])
            arrived(low.at[pl.ds(4, 4)], low_sem.at[2])
            for h in (2, 3, 4):
                @pl.when(y % 2 ** (h - 1) == 2 ** (h - 2) - 1)
                def _():
                    for k in (2, 1):
                        for c in low_copies(h):
                            for d in c[k]():
                                d.start()

        parts = (pl.ds(0, 2), pl.ds(2, 2), pl.ds(4, 4))

        def ring_copy(k, j):
            return remote(
                top.at[parts[k]], top.at[parts[k]], y_sem.at[k], top_sem.at[k], row, j * 2
            )

        def holds(h):
            return x % 2 == 0 if h == 5 else x == 1 if h == 6 else x == 3

        def along_x(h, k, src, side):
            first = x if h == 5 else 0
            for i in range(2 if h == 5 else 4):
                half = {5: i, 6: i // 2}.get(h, side)
                for d in table_copies(src, tab_sem.at[h - 5], h, z * N_X + first + i, peer, half)[k]():
                    yield d

        def along_z(h, k, places=None):
            size = 2 ** (h - 6)
            slots = mid.at[h - 7]
            for i in places or range(min(size, 4)):
                if i == size // 2 - 1:
                    continue
                to = ((z - z % size + i) * N_X + 3, y * 2)
                sems = (tab_sem.at[h - 5, k], mid_sem.at[h - 7, k])
                if k < 2:
                    yield remote(top.at[parts[k]], slots.at[parts[k]], *sems, *to)
                else:
                    side = i // (size // 2)
                    yield remote(top.at[4 + side], slots.at[4], *sems, *to)
                    yield remote(top.at[7 - side], slots.at[5], *sems, *to)

        def upper(k, heights):
            here = (row % 8 != 7) if heights[0] == 5 else (row % 8 == 7) & (row != 31)

            @pl.when(here)
            def _():
                arrived(top.at[parts[k]], top_sem.at[k], f"wait_top{k}")

                @pl.when(y == 7)
                def _():
                    for j in (2, 4, 0, 6):
                        ring_copy(k, j).start()

                @pl.when(relay == 1)
                def _():
                    ring_copy(k, jnp.where(y == 6, 5, y + 1)).start()

                for h in heights:
                    @pl.when(holds(h) if h < 7 else holds(h) & (z == keeper(h)))
                    def _():
                        if h >= 7:
                            for d in along_z(h, k):
                                d.start()
                        for d in along_x(h, k, top, 0):
                            d.start()

        def onward(k, h):
            @pl.when((x == 3) & (z != keeper(h)))
            def _():
                part = pl.ds(4, 2) if k == 2 else parts[k]
                arrived(mid.at[h - 7, part], mid_sem.at[h - 7, k], f"wait_mid{h}")
                for d in along_x(h, k, mid.at[h - 7], None):
                    d.start()

        def first_tables():
            upper(0, (5, 6, 7))
            upper(2, (8, 9))

        def local_work():
            loads[5].wait()
            loads[6].wait()
            for i in range(2):
                for r in range(4):
                    dense(i, r)
            loads[4].wait()
            arrived(r_f.at[1], rf_sem.at[1])
            for i in range(2):
                side_terms(i, vcp[1, 0], vcp[1, 3])

        @pl.when(y == 7)
        def _():
            first_tables()

        with jax.named_scope("local"):
            local_work()

        @pl.when(y != 7)
        def _():
            first_tables()

        with jax.named_scope("go"):
            pl.semaphore_wait(go_sem, 1)
        pl.when(y != 7)(low_rest)
        onward(0, 7)

        @pl.when(row == 15)
        def _():
            pl.semaphore_wait(mrdy_sem, 4)
            for d in along_z(9, 2, range(4, 8)):
                d.start()

        onward(2, 8)
        onward(2, 9)
        upper(2, (5, 6, 7))
        onward(2, 7)
        upper(1, (5, 6, 7))
        onward(1, 7)

        arrived(r_fin, fr_sem, "wait_fin")
        finish(r_fin[2], r_fin[0], r_fin[1])

        for c in mine:
            c.wait_send()

        @pl.when(y != 7)
        def _():
            for h in (2, 3, 4):
                @pl.when(y % 2 ** (h - 1) == 2 ** (h - 2) - 1)
                def _():
                    for k in range(3):
                        sent(acc.at[0, pl.ds(0, 32 * (1 if (h, k) == (2, 0) else 2 ** (h - 1)))], lows_sem.at[k])

        def drained(k, heights):
            here = (row % 8 != 7) if heights[0] == 5 else (row % 8 == 7) & (row != 31)

            @pl.when(here)
            def _():
                @pl.when(y == 7)
                def _():
                    sent(acc.at[0, pl.ds(0, 32 * 4 * (2 if k == 2 else 1))], y_sem.at[k])

                @pl.when(relay == 1)
                def _():
                    sent(acc.at[0, pl.ds(0, 32 * (2 if k == 2 else 1))], y_sem.at[k])

            for h in heights:
                if h < 7:
                    @pl.when(holds(h))
                    def _():
                        sent(acc.at[0, pl.ds(0, 32 * (2 if h == 5 else 4))], tab_sem.at[h - 5, k])
                    continue

                @pl.when((x == 3) & (z == keeper(h)))
                def _():
                    sent(acc.at[0, pl.ds(0, 32 * (4 + 2 ** (h - 6) - 1))], tab_sem.at[h - 5, k])

                @pl.when((x == 3) & (z != keeper(h)))
                def _():
                    sent(acc.at[0, pl.ds(0, 32 * 4)], tab_sem.at[h - 5, k])

        drained(0, (5, 6, 7))
        drained(1, (5, 6, 7))
        drained(2, (5, 6, 7))
        drained(2, (8, 9))

        @pl.when((y == 7) & (row % 8 == 7))
        def _():
            arrived(top.at[parts[0]], top_sem.at[0])
            arrived(top.at[parts[1]], top_sem.at[1])

        @pl.when((y == 7) & (row == 31))
        def _():
            arrived(top.at[parts[2]], top_sem.at[2])


def shards(dense_a, dense_b, inner, outer, ascent, descent, couplings):
    any_spec = pl.BlockSpec(memory_space=pl.ANY)
    dma = pltpu.SemaphoreType.DMA
    tile = (128, 128)
    return pl.pallas_call(
        kernel,
        out_shape=jax.ShapeDtypeStruct((2, 512, 512), BF),
        in_specs=[any_spec] * 7,
        out_specs=any_spec,
        scratch_shapes=[
            pltpu.VMEM((2, 512, 512), BF),
            pltpu.VMEM((2, 512, 512), BF),
            pltpu.VMEM((2, 2, 512, 128), BF),
            pltpu.VMEM((2, 2, 512, 128), BF),
            pltpu.VMEM((4, 2, *tile), BF),
            pltpu.VMEM((4, 2, *tile), BF),
            pltpu.VMEM((2, 4, *tile), BF),
            pltpu.VMEM((2, 512, 512), F32),
            pltpu.VMEM((2, 512, 512), BF),
            pltpu.VMEM((2, 512, 128), BF),
            pltpu.VMEM((2, 512, 128), BF),
            pltpu.VMEM((10, *tile), BF),
            pltpu.VMEM((10, *tile), BF),
            pltpu.VMEM((10, *tile), BF),
            pltpu.VMEM((10, *tile), BF),
            pltpu.VMEM((8, 2, *tile), BF),
            pltpu.VMEM((8, 2, *tile), BF),
            pltpu.VMEM((10, 2, *tile), BF),
            pltpu.VMEM((8, *tile), BF),
            pltpu.VMEM((8, *tile), BF),
            pltpu.VMEM((3, 6, *tile), BF),
            pltpu.VMEM((3, *tile), F32),
            pltpu.VMEM((3, *tile), F32),
            dma((7,)),
            dma,
            dma((10,)),
            dma((10,)),
            dma((10,)),
            dma((8,)),
            dma((8,)),
            dma((10,)),
            dma((1,)),
            dma((3,)),
            dma((3,)),
            dma((3, 3)),
            dma((3,)),
            dma((5, 3)),
            dma((3,)),
            dma((6,)),
            dma,
            dma,
            pltpu.SemaphoreType.REGULAR,
            pltpu.SemaphoreType.REGULAR,
            pltpu.SemaphoreType.REGULAR,
            dma,
        ],
        compiler_params=pltpu.CompilerParams(collective_id=0, has_side_effects=True),
        name="tree",
    )(dense_a, dense_b, inner, outer, ascent, descent, couplings)


def solution(mesh):
    placed = (
        P(("row", "col"), None, None),
        P(("row", "col"), None, None),
        P(("row", "col"), None, None, None),
        P(("row", "col"), None, None, None),
        P(("row", "col"), None, None, None, None),
        P(("row", "col"), None, None, None, None),
        P(("row", "col"), None, None, None, None),
    )
    return jax.shard_map(
        shards, mesh=mesh, in_specs=placed, out_specs=P(("row", "col"), None, None), check_vma=False
    )
```

```python
import jax
import jax.numpy as jnp
from jax import lax
from jax.experimental import pallas as pl
from jax.experimental.pallas import tpu as pltpu
from jax.sharding import PartitionSpec as P

MESH_ID = pl.DeviceIdType.MESH
BF = jnp.bfloat16
F32 = jnp.float32
N_X = 4
N_Y = 8
N_Z = 8
GO = 3
TOP = 9


def flip1(p):
    return p + 1 - 2 * (p % 2)


def flip3(p):
    return p - p % 4 + 3 - p % 4


def halves(v):
    if v.dtype == BF:
        return (v,)
    high = v.astype(BF)
    return high, (v - high.astype(F32)).astype(BF)


def product(a, b, ca, cb):
    a, b = halves(a), halves(b)
    terms = [(i, j) for i in range(len(a)) for j in range(len(b)) if i + j < 2]
    if len(terms) == 1:
        left, right = a[0], b[0]
    else:
        left = jnp.concatenate([a[i] for i, _ in terms], ca)
        right = jnp.concatenate([b[j] for _, j in terms], cb)
    return lax.dot_general(left, right, (((ca,), (cb,)), ((), ())), preferred_element_type=F32)


def mm(a, b):
    return product(a, b, 1, 0)


def mm_t0(a, b):
    return product(a, b, 0, 0)


def mm_t1(a, b):
    return product(a, b, 1, 1)


def kernel(
    da, db, ib, ob, asc, desc, cp, out,
    va, vb, vib, vob, vasc, vdesc, vcp,
    acc, us, vw, s_f, s_t, r_f, r_t,
    t_pq, t_sw, t_k, low, top, mid, s_fin, r_fin,
    ld_sem, xs_sem, rf_sem, rt_sem, rpq_sem, rsw_sem, rk_sem,
    hs_sem, low_sem, top_sem, mid_sem, y_sem, tab_sem, lows_sem, own_sem, fs_sem, fr_sem, go_sem, rdy_sem, mrdy_sem, hd_sem,
):
    row = lax.axis_index("row")
    col = lax.axis_index("col")
    z, x = row // N_X, row % N_X
    y, core = col // 2, col % 2

    def position(h):
        return y if h <= 4 else x if h <= 6 else z

    def route(h):
        p = position(h)
        if h in (2, 5, 7):
            return None, flip1(p), None
        if h == 6:
            return None, 3 - p, None
        middle = ((p + 1) // 2) % 2
        if h in (3, 8):
            near = flip3(p)
            return middle == 1, near, flip1(near)
        near = 7 - p
        return middle == 0, near, flip1(near)

    def sender(h, p):
        if h in (2, 5, 7):
            return flip1(p)
        if h == 6:
            return 3 - p
        middle = ((p + 1) // 2) % 2
        if h in (3, 8):
            return jnp.where(middle == 1, flip3(p), flip1(flip3(p)))
        return jnp.where(middle == 0, 7 - p, flip1(7 - p))

    def place(h, p, c):
        if h <= 4:
            return row, p * 2 + c
        if h <= 6:
            return z * N_X + p, y * 2 + c
        return p * N_X + x, y * 2 + c

    def keeper(h):
        size = 2 ** (h - 6)
        return z - z % size + size // 2 - 1

    loads = []
    pairs = ((ib, vib), (asc.at[0], vasc), (desc.at[0], vdesc), (cp.at[0], vcp), (ob, vob), (da, va), (db, vb))
    for i, (src, dst) in enumerate(pairs):
        c = pltpu.make_async_copy(src, dst, ld_sem.at[i])
        if i < 4:
            c.start()
        loads.append(c)

    barrier = pltpu.get_barrier_semaphore()

    def greet(r, c):
        pl.semaphore_signal(barrier, inc=1, device_id=(r, c), device_id_type=MESH_ID)

    middle_y, middle_z = ((y + 1) // 2) % 2, ((z + 1) // 2) % 2
    low_size = jnp.where(y % 2 == 0, 2, jnp.where(y % 4 == 1, 4, 8))
    below = jnp.where(z % 2 == 0, 1, jnp.where(z % 4 == 1, 3, jnp.where(z == 3, 3, 0)))
    upper_half = z // 4
    top_size = jnp.where(x % 2 == 0, 2, jnp.where(x == 1, 4, 12 + below))
    relay = jnp.where((y % 2 == 0) & (y != 4), 1, 0)

    @pl.when(core == 0)
    def _():
        greet(row, col + 1)
        pl.when(upper_half == 0)(lambda: greet(sender(TOP, z) * N_X + x, y * 2 + 1))

        for h in (7, 8, 9):
            @pl.when((x == 3) & (z != keeper(h)) & ((h < 9) | (upper_half == 0)))
            def _():
                greet(keeper(h) * N_X + 3, y * 2)

        @pl.when(row == 15)
        def _():
            for i in range(4, 8):
                greet(i * N_X + 3, y * 2)

        @pl.when(y != 7)
        def _():
            greet(row, jnp.where(y % 2 == 0, 7, jnp.where(y == 5, 6, y - 1)) * 2)

    @pl.when(core == 1)
    def _():
        greet(row, col - 1)
        for h in (2, 3, 4):
            keeps = y - y % 2 ** (h - 1) + 2 ** (h - 2) - 1
            greet(row, keeps * 2)
            pl.when(keeps != y)(lambda: greet(row, keeps * 2 + 1))
        for h in range(2, TOP):
            greet(*place(h, sender(h, position(h)), 1))
        pl.when(upper_half == 0)(lambda: greet(*place(TOP, sender(TOP, z), 1)))

        @pl.when((upper_half == 0) & (middle_z == 0))
        def _():
            for c in (0, 1):
                greet(*place(TOP, 7 - z, c))
                greet(*place(TOP, flip1(7 - z), c))

        for holder in (x - x % 2, 1, 3, 3, 3):
            greet(z * N_X + holder, y * 2)

    receivers = jnp.where(
        core == 0,
        1 + jnp.where(y == 7, 4, low_size) + relay + top_size + upper_half * (1 + x // 3),
        5 + 2 + jnp.where(y == 7, 0, low_size - 1) + 2 * middle_z + upper_half * (4 * (1 - middle_z) + 1),
    )

    with jax.named_scope("load"):
        loads[1].wait()
        up = [mm(vasc[i, 0], vasc[2, 0]) for i in range(2)], [mm(vasc[i, 1], vasc[2, 1]) for i in range(2)]
        loads[0].wait()
        for c in loads[4:]:
            c.start()
    leaf = [mm_t0(vib[i, 0], vib[i, 1]) for i in range(2)]
    lifted = sum(mm(mm_t0(up[0][i], leaf[i]), up[1][i]) for i in range(2))
    s_t[1] = lifted.astype(BF)
    node = sum(mm(mm_t0(vasc[i, 0], leaf[i]), vasc[i, 1]) for i in range(2))
    s_f[1] = node.astype(BF)

    with jax.named_scope("entry"):
        pl.semaphore_wait(barrier, receivers)

    @pl.when(upper_half == 1)
    def _():
        pl.semaphore_signal(rdy_sem, inc=1, device_id=place(TOP, sender(TOP, z), 1), device_id_type=MESH_ID)

        @pl.when((core == 0) & (x == 3))
        def _():
            pl.semaphore_signal(mrdy_sem, inc=1, device_id=(15, y * 2), device_id_type=MESH_ID)

    def remote(src, dst, ssem, rsem, r, c):
        return pltpu.make_async_remote_copy(
            src_ref=src, dst_ref=dst, send_sem=ssem, recv_sem=rsem,
            device_id=(r, c), device_id_type=MESH_ID,
        )

    def arrived(dst, sem, name="wait"):
        with jax.named_scope(name):
            remote(dst, dst, xs_sem.at[0], sem, row, col).wait_recv()

    def sent(src, sem):
        remote(src, src, sem, rf_sem.at[0], row, col).wait_send()

    def dense(i, r):
        rows = pl.ds(r * 128, 128)
        acc[i, rows, :] = jnp.dot(va[i, rows, :], vb[i], preferred_element_type=F32)

    def side_terms(i, kl1, kr1):
        near_node = mm(mm(kl1, r_f[1]), kr1)
        if True:
            kl, kr = (vcp[0, 0], vcp[0, 3]) if i == 0 else (vcp[0, 1], vcp[0, 2])
            g = mm(mm(kl, leaf[1 - i]), kr)
            g = g + mm_t1(mm(vdesc[i, 0], near_node), vdesc[i, 1])
            us[i] = mm(vob[i, 0], mm(vdesc[i, 0], vdesc[2, 0])).astype(BF)
            vw[i] = mm(vob[i, 1], mm(vdesc[i, 1], vdesc[2, 1])).astype(BF)
            acc[i] += mm_t1(mm(vob[i, 0], g.astype(BF)).astype(BF), vob[i, 1])

    def finish(g, left, right):
        arrived(r_f.at[TOP], rf_sem.at[TOP], "wait_f9")
        g = (g + mm(mm(left, r_f[TOP]), right)).astype(BF)
        for i in range(2):
            spread = mm(us[i], g).astype(BF)
            for r in range(2):
                rows = pl.ds(r * 256, 256)
                block = acc[i, rows, :] + mm_t1(spread[r * 256:(r + 1) * 256], vw[i])
                out[i, rows, :] = block.astype(BF)

    def when(cond, f):
        if cond is None:
            f()
        else:
            pl.when(cond)(f)

    def send_f(h, p, c):
        r, cc = place(h, p, c)
        return remote(s_f.at[h], r_f.at[h], xs_sem.at[h], rf_sem.at[h], r, cc)

    def send_t(h, p):
        r, cc = place(h, p, 1)
        return remote(s_t.at[h], r_t.at[h], xs_sem.at[h], rt_sem.at[h], r, cc)

    def table_copies(src, sem, h, r, c, side):
        return (
            lambda: (remote(src.at[pl.ds(0, 2)], t_pq.at[h], sem.at[0], rpq_sem.at[h], r, c),),
            lambda: (remote(src.at[pl.ds(2, 2)], t_sw.at[h], sem.at[1], rsw_sem.at[h], r, c),),
            lambda: (
                remote(src.at[4 if side is None else 4 + side], t_k.at[h, 0], sem.at[2], rk_sem.at[h], r, c),
                remote(src.at[5 if side is None else 7 - side], t_k.at[h, 1], sem.at[2], rk_sem.at[h], r, c),
            ),
        )

    @pl.when(core == 1)
    def _():
        me_c = y * 2 + 1
        send = remote(s_f.at[1], r_f.at[1], xs_sem.at[1], rf_sem.at[1], row, me_c - 1)
        send.start()
        loads[2].wait()
        loads[3].wait()

        def hand_over(dst, sems):
            return [
                remote(vasc.at[3], dst.at[pl.ds(0, 2)], hs_sem.at[0], sems.at[0], row, me_c - 1),
                remote(vdesc.at[3], dst.at[pl.ds(2, 2)], hs_sem.at[0], sems.at[1], row, me_c - 1),
                remote(vcp.at[1], dst.at[pl.ds(4, 4)], hs_sem.at[0], sems.at[2], row, me_c - 1),
            ]

        def hand_all():
            @pl.when(y == 7)
            def _():
                for c in hand_over(top, top_sem):
                    c.start()

            @pl.when(y != 7)
            def _():
                for c in hand_over(low, low_sem)[1:]:
                    c.start()

        def ahead(h):
            size = 2 ** (h - 1)
            base = y - y % size
            order = {2: (1,), 3: (3, 0, 2), 4: (7, 0, 6, 1, 5, 2, 4)}[h]
            own = pltpu.make_async_copy(vasc.at[3], t_pq.at[h], rpq_sem.at[h])
            return own, [
                remote(vasc.at[3], t_pq.at[h], hd_sem, rpq_sem.at[h], row, (base + i) * 2 + 1) for i in order
            ]

        for h in (2, 3, 4):
            @pl.when(y % 2 ** (h - 1) == 2 ** (h - 2) - 1)
            def _():
                own, others = ahead(h)
                for c in others:
                    c.start()
                own.start()

        hand_all()
        down = {}

        def compose(h):
            arrived(t_k.at[h], rk_sem.at[h], f"wait_k{h}")
            left, right = t_k[h, 0], t_k[h, 1]
            if h >= 3:
                arrived(t_sw.at[h - 2], rsw_sem.at[h - 2], f"wait_sw{h - 2}")
                s, w = t_sw[h - 2, 0], t_sw[h - 2, 1]
                if h == 3:
                    down["s"], down["w"] = s, w.T
                else:
                    down["s"] = mm(down["s"], s)
                    down["w"] = mm_t0(w, down["w"])
                left = mm(down["s"], left)
                right = mm(right, down["w"])
            if h == TOP:
                return left, right
            arrived(r_f.at[h], rf_sem.at[h], f"wait_f{h}")
            g = mm(mm(left, r_f[h]), right)
            down["g"] = g if h == 2 else down["g"] + g

        def filler(h):
            if h == 2:
                loads[5].wait()
                loads[6].wait()
                for r in range(4):
                    dense(0, r)
            if h == 3:
                for r in range(4):
                    dense(1, r)
                arrived(t_k.at[1], rk_sem.at[1])
                loads[4].wait()
                side_terms(0, t_k[1, 0], t_k[1, 1])
            if h == 4:
                side_terms(1, t_k[1, 0], t_k[1, 1])
            if h == 7:
                compose(2)
                compose(3)
            if h == 8:
                compose(4)

        arrived(r_f.at[1], rf_sem.at[1])
        arrived(r_t.at[1], rt_sem.at[1], "wait_t1")
        current = lifted + r_t[1].astype(F32)
        for h in range(2, TOP + 1):
            cond, near, far = route(h)
            s_f[h] = current.astype(BF)
            if h == TOP:
                def go():
                    pl.when(upper_half == 0)(lambda: pl.semaphore_wait(rdy_sem, 4))
                    for p, c in ((far, 1), (near, 1), (far, 0), (near, 0)):
                        send_f(h, p, c).start()
                when(cond, go)
                break
            arrived(t_pq.at[h - 1], rpq_sem.at[h - 1], f"wait_pq{h - 1}")
            term = mm(mm_t0(t_pq[h - 1, 0], current), t_pq[h - 1, 1])
            s_t[h] = term.astype(BF)

            def go():
                if far is not None:
                    send_t(h, far).start()
                send_t(h, near).start()
                if far is not None:
                    send_f(h, far, 1).start()
                send_f(h, near, 1).start()
            when(cond, go)
            with jax.named_scope(f"fill{h}"):
                filler(h)
            arrived(r_t.at[h], rt_sem.at[h], f"wait_t{h}")
            current = term + r_t[h].astype(F32)
            if h == GO:
                pl.semaphore_signal(go_sem, inc=1, device_id=(row, me_c - 1), device_id_type=MESH_ID)
        compose(5)
        compose(6)
        compose(7)
        compose(8)
        left, right = compose(9)
        s_fin[0] = left
        s_fin[1] = right
        s_fin[2] = down["g"]
        fin = remote(s_fin, r_fin, fs_sem, fr_sem, row, me_c - 1)
        fin.start()
        finish(down["g"], left, right)
        send.wait_send()
        for h in (2, 3, 4):
            @pl.when(y % 2 ** (h - 1) == 2 ** (h - 2) - 1)
            def _():
                sent(acc.at[0, pl.ds(0, 32 * (2 ** (h - 1) - 1))], hd_sem)
        fin.wait_send()
        pl.when(y == 7)(lambda: sent(top, hs_sem.at[0]))
        pl.when(y != 7)(lambda: sent(low.at[pl.ds(2, 6)], hs_sem.at[0]))
        for h in range(2, TOP + 1):
            cond, near, far = route(h)
            count = 2 if far is None else 4
            when(cond, lambda: sent(s_f.at[pl.ds(0, count)], xs_sem.at[h]))

    @pl.when(core == 0)
    def _():
        peer = y * 2 + 1
        mine = [
            remote(s_t.at[1], r_t.at[1], own_sem.at[0], rt_sem.at[1], row, peer),
            remote(s_f.at[1], r_f.at[1], own_sem.at[1], rf_sem.at[1], row, peer),
            remote(vasc.at[3], t_pq.at[1], own_sem.at[2], rpq_sem.at[1], row, peer),
        ]
        for c in mine:
            c.start()
        loads[2].wait()
        loads[3].wait()
        more = [
            remote(vdesc.at[3], t_sw.at[1], own_sem.at[3], rsw_sem.at[1], row, peer),
            remote(vcp.at[1, 1], t_k.at[1, 0], own_sem.at[4], rk_sem.at[1], row, peer),
            remote(vcp.at[1, 2], t_k.at[1, 1], own_sem.at[5], rk_sem.at[1], row, peer),
        ]
        for c in more:
            c.start()
        mine += more

        def low_copies(h):
            size = 2 ** (h - 1)
            base = y - y % size
            for i in range(size):
                yield table_copies(low, lows_sem, h, row, (base + i) * 2 + 1, i // (size // 2))

        def low_rest():
            arrived(low.at[pl.ds(2, 2)], low_sem.at[1])
            arrived(low.at[pl.ds(4, 4)], low_sem.at[2])
            for h in (2, 3, 4):
                @pl.when(y % 2 ** (h - 1) == 2 ** (h - 2) - 1)
                def _():
                    for k in (2, 1):
                        for c in low_copies(h):
                            for d in c[k]():
                                d.start()

        parts = (pl.ds(0, 2), pl.ds(2, 2), pl.ds(4, 4))

        def ring_copy(k, j):
            return remote(
                top.at[parts[k]], top.at[parts[k]], y_sem.at[k], top_sem.at[k], row, j * 2
            )

        def holds(h):
            return x % 2 == 0 if h == 5 else x == 1 if h == 6 else x == 3

        def along_x(h, k, src, side):
            first = x if h == 5 else 0
            for i in range(2 if h == 5 else 4):
                half = {5: i, 6: i // 2}.get(h, side)
                for d in table_copies(src, tab_sem.at[h - 5], h, z * N_X + first + i, peer, half)[k]():
                    yield d

        def along_z(h, k, places=None):
            size = 2 ** (h - 6)
            slots = mid.at[h - 7]
            for i in places or range(min(size, 4)):
                if i == size // 2 - 1:
                    continue
                to = ((z - z % size + i) * N_X + 3, y * 2)
                sems = (tab_sem.at[h - 5, k], mid_sem.at[h - 7, k])
                if k < 2:
                    yield remote(top.at[parts[k]], slots.at[parts[k]], *sems, *to)
                else:
                    side = i // (size // 2)
                    yield remote(top.at[4 + side], slots.at[4], *sems, *to)
                    yield remote(top.at[7 - side], slots.at[5], *sems, *to)

        def upper(k, heights):
            here = (row % 8 != 7) if heights[0] == 5 else (row % 8 == 7) & (row != 31)

            @pl.when(here)
            def _():
                arrived(top.at[parts[k]], top_sem.at[k], f"wait_top{k}")

                @pl.when(y == 7)
                def _():
                    for j in (2, 4, 0, 6):
                        ring_copy(k, j).start()

                @pl.when(relay == 1)
                def _():
                    ring_copy(k, jnp.where(y == 6, 5, y + 1)).start()

                for h in heights:
                    @pl.when(holds(h) if h < 7 else holds(h) & (z == keeper(h)))
                    def _():
                        if h >= 7:
                            for d in along_z(h, k):
                                d.start()
                        for d in along_x(h, k, top, 0):
                            d.start()

        def onward(k, h):
            @pl.when((x == 3) & (z != keeper(h)))
            def _():
                part = pl.ds(4, 2) if k == 2 else parts[k]
                arrived(mid.at[h - 7, part], mid_sem.at[h - 7, k], f"wait_mid{h}")
                for d in along_x(h, k, mid.at[h - 7], None):
                    d.start()

        def first_tables():
            upper(0, (5, 6, 7))
            upper(2, (8, 9))

        def local_work():
            loads[5].wait()
            loads[6].wait()
            for i in range(2):
                for r in range(4):
                    dense(i, r)
            loads[4].wait()
            arrived(r_f.at[1], rf_sem.at[1])
            for i in range(2):
                side_terms(i, vcp[1, 0], vcp[1, 3])

        @pl.when(y == 7)
        def _():
            first_tables()

        with jax.named_scope("local"):
            local_work()

        @pl.when(y != 7)
        def _():
            first_tables()

        with jax.named_scope("go"):
            pl.semaphore_wait(go_sem, 1)
        pl.when(y != 7)(low_rest)
        onward(0, 7)

        @pl.when(row == 15)
        def _():
            pl.semaphore_wait(mrdy_sem, 4)
            for d in along_z(9, 2, range(4, 8)):
                d.start()

        onward(2, 8)
        onward(2, 9)
        upper(2, (5, 6, 7))
        onward(2, 7)
        upper(1, (5, 6, 7))
        onward(1, 7)

        arrived(r_fin, fr_sem, "wait_fin")
        finish(r_fin[2], r_fin[0], r_fin[1])

        for c in mine:
            c.wait_send()

        @pl.when(y != 7)
        def _():
            for h in (2, 3, 4):
                @pl.when(y % 2 ** (h - 1) == 2 ** (h - 2) - 1)
                def _():
                    for k in (1, 2):
                        sent(acc.at[0, pl.ds(0, 32 * 2 ** (h - 1))], lows_sem.at[k])

        def drained(k, heights):
            here = (row % 8 != 7) if heights[0] == 5 else (row % 8 == 7) & (row != 31)

            @pl.when(here)
            def _():
                @pl.when(y == 7)
                def _():
                    sent(acc.at[0, pl.ds(0, 32 * 4 * (2 if k == 2 else 1))], y_sem.at[k])

                @pl.when(relay == 1)
                def _():
                    sent(acc.at[0, pl.ds(0, 32 * (2 if k == 2 else 1))], y_sem.at[k])

            for h in heights:
                if h < 7:
                    @pl.when(holds(h))
                    def _():
                        sent(acc.at[0, pl.ds(0, 32 * (2 if h == 5 else 4))], tab_sem.at[h - 5, k])
                    continue

                @pl.when((x == 3) & (z == keeper(h)))
                def _():
                    sent(acc.at[0, pl.ds(0, 32 * (4 + 2 ** (h - 6) - 1))], tab_sem.at[h - 5, k])

                @pl.when((x == 3) & (z != keeper(h)))
                def _():
                    sent(acc.at[0, pl.ds(0, 32 * 4)], tab_sem.at[h - 5, k])

        drained(0, (5, 6, 7))
        drained(1, (5, 6, 7))
        drained(2, (5, 6, 7))
        drained(2, (8, 9))

        @pl.when((y == 7) & (row % 8 == 7))
        def _():
            arrived(top.at[parts[0]], top_sem.at[0])
            arrived(top.at[parts[1]], top_sem.at[1])

        @pl.when((y == 7) & (row == 31))
        def _():
            arrived(top.at[parts[2]], top_sem.at[2])


def shards(dense_a, dense_b, inner, outer, ascent, descent, couplings):
    dma = pltpu.SemaphoreType.DMA
    tile = (128, 128)
    return pl.pallas_call(
        kernel,
        out_shape=pltpu.VMEM((2, 512, 512), BF),
        in_specs=[pl.BlockSpec(memory_space=pltpu.HBM)] * 7,
        out_specs=pl.BlockSpec(memory_space=pltpu.VMEM),
        scratch_shapes=[
            pltpu.VMEM((2, 512, 512), BF),
            pltpu.VMEM((2, 512, 512), BF),
            pltpu.VMEM((2, 2, 512, 128), BF),
            pltpu.VMEM((2, 2, 512, 128), BF),
            pltpu.VMEM((4, 2, *tile), BF),
            pltpu.VMEM((4, 2, *tile), BF),
            pltpu.VMEM((2, 4, *tile), BF),
            pltpu.VMEM((2, 512, 512), F32),
            pltpu.VMEM((2, 512, 128), BF),
            pltpu.VMEM((2, 512, 128), BF),
            pltpu.VMEM((10, *tile), BF),
            pltpu.VMEM((10, *tile), BF),
            pltpu.VMEM((10, *tile), BF),
            pltpu.VMEM((10, *tile), BF),
            pltpu.VMEM((8, 2, *tile), BF),
            pltpu.VMEM((8, 2, *tile), BF),
            pltpu.VMEM((10, 2, *tile), BF),
            pltpu.VMEM((8, *tile), BF),
            pltpu.VMEM((8, *tile), BF),
            pltpu.VMEM((3, 6, *tile), BF),
            pltpu.VMEM((3, *tile), F32),
            pltpu.VMEM((3, *tile), F32),
            dma((7,)),
            dma((10,)),
            dma((10,)),
            dma((10,)),
            dma((8,)),
            dma((8,)),
            dma((10,)),
            dma((1,)),
            dma((3,)),
            dma((3,)),
            dma((3, 3)),
            dma((3,)),
            dma((5, 3)),
            dma((3,)),
            dma((6,)),
            dma,
            dma,
            pltpu.SemaphoreType.REGULAR,
            pltpu.SemaphoreType.REGULAR,
            pltpu.SemaphoreType.REGULAR,
            dma,
        ],
        compiler_params=pltpu.CompilerParams(collective_id=0, has_side_effects=True, vmem_limit_bytes=24 * 2**20),
        name="tree",
    )(*[pltpu.with_memory_space_constraint(v, pltpu.HBM) for v in (dense_a, dense_b, inner, outer, ascent, descent, couplings)])


def solution(mesh):
    placed = (
        P(("row", "col"), None, None),
        P(("row", "col"), None, None),
        P(("row", "col"), None, None, None),
        P(("row", "col"), None, None, None),
        P(("row", "col"), None, None, None, None),
        P(("row", "col"), None, None, None, None),
        P(("row", "col"), None, None, None, None),
    )
    return jax.shard_map(
        shards, mesh=mesh, in_specs=placed, out_specs=P(("row", "col"), None, None), check_vma=False
    )
```

```python
import jax
import jax.numpy as jnp
from jax import lax
from jax.experimental import pallas as pl
from jax.experimental.pallas import tpu as pltpu
from jax.sharding import PartitionSpec as P

MESH_ID = pl.DeviceIdType.MESH
BF = jnp.bfloat16
F32 = jnp.float32
N_X = 4
N_Y = 8
N_Z = 8
GO = 3
TOP = 9


def flip1(p):
    return p + 1 - 2 * (p % 2)


def flip3(p):
    return p - p % 4 + 3 - p % 4


def halves(v):
    if v.dtype == BF:
        return (v,)
    high = v.astype(BF)
    return high, (v - high.astype(F32)).astype(BF)


def product(a, b, ca, cb):
    a, b = halves(a), halves(b)
    terms = [(i, j) for i in range(len(a)) for j in range(len(b)) if i + j < 2]
    if len(terms) == 1:
        left, right = a[0], b[0]
    else:
        left = jnp.concatenate([a[i] for i, _ in terms], ca)
        right = jnp.concatenate([b[j] for _, j in terms], cb)
    return lax.dot_general(left, right, (((ca,), (cb,)), ((), ())), preferred_element_type=F32)


def mm(a, b):
    return product(a, b, 1, 0)


def mm_t0(a, b):
    return product(a, b, 0, 0)


def mm_t1(a, b):
    return product(a, b, 1, 1)


def kernel(
    da, db, ib, ob, asc, desc, cp, out,
    va, vb, vib, vob, vasc, vdesc, vcp,
    acc, us, vw, bw, s_f, s_t, r_f, r_t,
    t_pq, t_sw, t_k, low, top, mid, s_fin, r_fin,
    ld_sem, xs_sem, rf_sem, rt_sem, rpq_sem, rsw_sem, rk_sem,
    hs_sem, low_sem, top_sem, mid_sem, y_sem, tab_sem, lows_sem, own_sem, fs_sem, fr_sem, go_sem, rdy_sem, mrdy_sem, hd_sem,
):
    row = lax.axis_index("row")
    col = lax.axis_index("col")
    z, x = row // N_X, row % N_X
    y, core = col // 2, col % 2

    def position(h):
        return y if h <= 4 else x if h <= 6 else z

    def route(h):
        p = position(h)
        if h in (2, 5, 7):
            return None, flip1(p), None
        if h == 6:
            return None, 3 - p, None
        middle = ((p + 1) // 2) % 2
        if h in (3, 8):
            near = flip3(p)
            return middle == 1, near, flip1(near)
        near = 7 - p
        return middle == 0, near, flip1(near)

    def sender(h, p):
        if h in (2, 5, 7):
            return flip1(p)
        if h == 6:
            return 3 - p
        middle = ((p + 1) // 2) % 2
        if h in (3, 8):
            return jnp.where(middle == 1, flip3(p), flip1(flip3(p)))
        return jnp.where(middle == 0, 7 - p, flip1(7 - p))

    def place(h, p, c):
        if h <= 4:
            return row, p * 2 + c
        if h <= 6:
            return z * N_X + p, y * 2 + c
        return p * N_X + x, y * 2 + c

    def keeper(h):
        size = 2 ** (h - 6)
        return z - z % size + size // 2 - 1

    loads = []
    pairs = ((ib, vib), (asc.at[0], vasc), (desc.at[0], vdesc), (cp.at[0], vcp), (ob, vob), (da, va), (db, vb))
    for i, (src, dst) in enumerate(pairs):
        loads.append(pltpu.make_async_copy(src, dst, ld_sem.at[i]))
    for i in (1, 0):
        loads[i].start()

    barrier = pltpu.get_barrier_semaphore()

    def greet(r, c):
        pl.semaphore_signal(barrier, inc=1, device_id=(r, c), device_id_type=MESH_ID)

    middle_y, middle_z = ((y + 1) // 2) % 2, ((z + 1) // 2) % 2
    low_size = jnp.where(y % 2 == 0, 2, jnp.where(y % 4 == 1, 4, 8))
    below = jnp.where(z % 2 == 0, 1, jnp.where(z % 4 == 1, 3, jnp.where(z == 3, 3, 0)))
    upper_half = z // 4
    top_size = jnp.where(x % 2 == 0, 2, jnp.where(x == 1, 4, 12 + below))
    relay = jnp.where((y % 2 == 0) & (y != 4), 1, 0)

    @pl.when(core == 0)
    def _():
        greet(row, col + 1)
        pl.when(upper_half == 0)(lambda: greet(sender(TOP, z) * N_X + x, y * 2 + 1))

        for h in (7, 8, 9):
            @pl.when((x == 3) & (z != keeper(h)) & ((h < 9) | (upper_half == 0)))
            def _():
                greet(keeper(h) * N_X + 3, y * 2)

        @pl.when(row == 15)
        def _():
            for i in range(4, 8):
                greet(i * N_X + 3, y * 2)

        @pl.when(y != 7)
        def _():
            greet(row, jnp.where(y % 2 == 0, 7, jnp.where(y == 5, 6, y - 1)) * 2)

    @pl.when(core == 1)
    def _():
        greet(row, col - 1)
        for h in (2, 3, 4):
            keeps = y - y % 2 ** (h - 1) + 2 ** (h - 2) - 1
            greet(row, keeps * 2)
            pl.when(keeps != y)(lambda: greet(row, keeps * 2 + 1))
        for h in range(2, TOP):
            greet(*place(h, sender(h, position(h)), 1))
        pl.when(upper_half == 0)(lambda: greet(*place(TOP, sender(TOP, z), 1)))

        @pl.when((upper_half == 0) & (middle_z == 0))
        def _():
            for c in (0, 1):
                greet(*place(TOP, 7 - z, c))
                greet(*place(TOP, flip1(7 - z), c))

        for holder in (x - x % 2, 1, 3, 3, 3):
            greet(z * N_X + holder, y * 2)

    receivers = jnp.where(
        core == 0,
        1 + jnp.where(y == 7, 4, low_size) + relay + top_size + upper_half * (1 + x // 3),
        5 + 2 + jnp.where(y == 7, 0, low_size - 1) + 2 * middle_z + upper_half * (4 * (1 - middle_z) + 1),
    )

    with jax.named_scope("load"):
        loads[1].wait()
        up = [mm(vasc[i, 0], vasc[2, 0]) for i in range(2)], [mm(vasc[i, 1], vasc[2, 1]) for i in range(2)]
        loads[0].wait()
        for c in loads[2:]:
            c.start()
    leaf = [mm_t0(vib[i, 0], vib[i, 1]) for i in range(2)]
    lifted = sum(mm(mm_t0(up[0][i], leaf[i]), up[1][i]) for i in range(2))
    s_t[1] = lifted.astype(BF)
    node = sum(mm(mm_t0(vasc[i, 0], leaf[i]), vasc[i, 1]) for i in range(2))
    s_f[1] = node.astype(BF)

    with jax.named_scope("entry"):
        pl.semaphore_wait(barrier, receivers)

    @pl.when(upper_half == 1)
    def _():
        pl.semaphore_signal(rdy_sem, inc=1, device_id=place(TOP, sender(TOP, z), 1), device_id_type=MESH_ID)

        @pl.when((core == 0) & (x == 3))
        def _():
            pl.semaphore_signal(mrdy_sem, inc=1, device_id=(15, y * 2), device_id_type=MESH_ID)

    def remote(src, dst, ssem, rsem, r, c):
        return pltpu.make_async_remote_copy(
            src_ref=src, dst_ref=dst, send_sem=ssem, recv_sem=rsem,
            device_id=(r, c), device_id_type=MESH_ID,
        )

    def arrived(dst, sem, name="wait"):
        with jax.named_scope(name):
            remote(dst, dst, xs_sem.at[0], sem, row, col).wait_recv()

    def sent(src, sem):
        remote(src, src, sem, rf_sem.at[0], row, col).wait_send()

    def dense(i, r):
        rows = pl.ds(r * 128, 128)
        acc[i, rows, :] = jnp.dot(va[i, rows, :], vb[i], preferred_element_type=F32)

    def side_terms(i, kl1, kr1):
        near_node = mm(mm(kl1, r_f[1]), kr1)
        if True:
            kl, kr = (vcp[0, 0], vcp[0, 3]) if i == 0 else (vcp[0, 1], vcp[0, 2])
            g = mm(mm(kl, leaf[1 - i]), kr)
            g = g + mm_t1(mm(vdesc[i, 0], near_node), vdesc[i, 1])
            us[i] = mm(vob[i, 0], mm(vdesc[i, 0], vdesc[2, 0])).astype(BF)
            vw[i] = mm(vob[i, 1], mm(vdesc[i, 1], vdesc[2, 1])).astype(BF)
            acc[i] += mm_t1(mm(vob[i, 0], g.astype(BF)).astype(BF), vob[i, 1])

    def prepare(g, left, right):
        for i in range(2):
            acc[i] += mm_t1(mm(us[i], g.astype(BF)).astype(BF), vw[i])
            us[i] = mm(us[i], left).astype(BF)
            bw[i] = mm_t1(right, vw[i]).astype(BF)

    def finish():
        arrived(r_f.at[TOP], rf_sem.at[TOP], "wait_f9")
        for i in range(2):
            spread = mm(us[i], r_f[TOP]).astype(BF)
            for r in range(2):
                rows = pl.ds(r * 256, 256)
                block = acc[i, rows, :] + mm(spread[r * 256:(r + 1) * 256], bw[i])
                out[i, rows, :] = block.astype(BF)

    def when(cond, f):
        if cond is None:
            f()
        else:
            pl.when(cond)(f)

    def send_f(h, p, c):
        r, cc = place(h, p, c)
        return remote(s_f.at[h], r_f.at[h], xs_sem.at[h], rf_sem.at[h], r, cc)

    def send_t(h, p):
        r, cc = place(h, p, 1)
        return remote(s_t.at[h], r_t.at[h], xs_sem.at[h], rt_sem.at[h], r, cc)

    def table_copies(src, sem, h, r, c, side):
        return (
            lambda: (remote(src.at[pl.ds(0, 2)], t_pq.at[h], sem.at[0], rpq_sem.at[h], r, c),),
            lambda: (remote(src.at[pl.ds(2, 2)], t_sw.at[h], sem.at[1], rsw_sem.at[h], r, c),),
            lambda: (
                remote(src.at[4 if side is None else 4 + side], t_k.at[h, 0], sem.at[2], rk_sem.at[h], r, c),
                remote(src.at[5 if side is None else 7 - side], t_k.at[h, 1], sem.at[2], rk_sem.at[h], r, c),
            ),
        )

    @pl.when(core == 1)
    def _():
        me_c = y * 2 + 1
        send = remote(s_f.at[1], r_f.at[1], xs_sem.at[1], rf_sem.at[1], row, me_c - 1)
        send.start()
        loads[2].wait()
        loads[3].wait()

        def hand_over(dst, sems):
            return [
                remote(vasc.at[3], dst.at[pl.ds(0, 2)], hs_sem.at[0], sems.at[0], row, me_c - 1),
                remote(vdesc.at[3], dst.at[pl.ds(2, 2)], hs_sem.at[0], sems.at[1], row, me_c - 1),
                remote(vcp.at[1], dst.at[pl.ds(4, 4)], hs_sem.at[0], sems.at[2], row, me_c - 1),
            ]

        def hand_all():
            @pl.when(y == 7)
            def _():
                for c in hand_over(top, top_sem):
                    c.start()

            @pl.when(y != 7)
            def _():
                for c in hand_over(low, low_sem)[1:]:
                    c.start()

        def ahead(h):
            size = 2 ** (h - 1)
            base = y - y % size
            order = {2: (1,), 3: (3, 0, 2), 4: (7, 0, 6, 1, 5, 2, 4)}[h]
            own = pltpu.make_async_copy(vasc.at[3], t_pq.at[h], rpq_sem.at[h])
            return own, [
                remote(vasc.at[3], t_pq.at[h], hd_sem, rpq_sem.at[h], row, (base + i) * 2 + 1) for i in order
            ]

        def spread_ahead(heights):
            for h in heights:
                @pl.when(y % 2 ** (h - 1) == 2 ** (h - 2) - 1)
                def _():
                    own, others = ahead(h)
                    for c in others:
                        c.start()
                    own.start()

        spread_ahead((2,))
        hand_all()
        down = {}

        def compose(h):
            arrived(t_k.at[h], rk_sem.at[h], f"wait_k{h}")
            left, right = t_k[h, 0], t_k[h, 1]
            if h >= 3:
                arrived(t_sw.at[h - 2], rsw_sem.at[h - 2], f"wait_sw{h - 2}")
                s, w = t_sw[h - 2, 0], t_sw[h - 2, 1]
                if h == 3:
                    down["s"], down["w"] = s, w.T
                else:
                    down["s"] = mm(down["s"], s)
                    down["w"] = mm_t0(w, down["w"])
                left = mm(down["s"], left)
                right = mm(right, down["w"])
            if h == TOP:
                return left, right
            arrived(r_f.at[h], rf_sem.at[h], f"wait_f{h}")
            g = mm(mm(left, r_f[h]), right)
            down["g"] = g if h == 2 else down["g"] + g

        def filler(h):
            if h == 2:
                loads[5].wait()
                loads[6].wait()
                for r in range(4):
                    dense(0, r)
            if h == 3:
                for r in range(4):
                    dense(1, r)
                arrived(t_k.at[1], rk_sem.at[1])
                loads[4].wait()
                side_terms(0, t_k[1, 0], t_k[1, 1])
            if h == 4:
                side_terms(1, t_k[1, 0], t_k[1, 1])
            if h == 7:
                compose(2)
                compose(3)
            if h == 8:
                compose(4)

        arrived(r_f.at[1], rf_sem.at[1])
        arrived(r_t.at[1], rt_sem.at[1], "wait_t1")
        current = lifted + r_t[1].astype(F32)
        for h in range(2, TOP + 1):
            cond, near, far = route(h)
            s_f[h] = current.astype(BF)
            if h == TOP:
                def go():
                    pl.when(upper_half == 0)(lambda: pl.semaphore_wait(rdy_sem, 4))
                    for p, c in ((near, 1), (near, 0), (far, 1), (far, 0)):
                        send_f(h, p, c).start()
                when(cond, go)
                break
            if h == 2:
                arrived(t_pq.at[1], rpq_sem.at[1], "wait_pq1")
                term = mm(mm_t0(t_pq[1, 0], current), t_pq[1, 1])
            else:
                term = mm(mm(turned, current), t_pq[h - 1, 1])
            s_t[h] = term.astype(BF)

            def go():
                if far is not None:
                    send_t(h, far).start()
                send_t(h, near).start()
                if far is not None:
                    send_f(h, far, 1).start()
                send_f(h, near, 1).start()
            when(cond, go)
            if h == 2:
                spread_ahead((3, 4))
            with jax.named_scope(f"fill{h}"):
                filler(h)
            if h < TOP - 1:
                arrived(t_pq.at[h], rpq_sem.at[h], f"wait_pq{h}")
                turned = t_pq[h, 0].T
            arrived(r_t.at[h], rt_sem.at[h], f"wait_t{h}")
            current = term + r_t[h].astype(F32)
            if h == GO:
                pl.semaphore_signal(go_sem, inc=1, device_id=(row, me_c - 1), device_id_type=MESH_ID)
        compose(5)
        compose(6)
        compose(7)
        compose(8)
        left, right = compose(9)
        s_fin[0] = left
        s_fin[1] = right
        s_fin[2] = down["g"]
        fin = remote(s_fin, r_fin, fs_sem, fr_sem, row, me_c - 1)
        fin.start()
        prepare(down["g"], left, right)
        send.wait_send()
        for h in (2, 3, 4):
            @pl.when(y % 2 ** (h - 1) == 2 ** (h - 2) - 1)
            def _():
                sent(acc.at[0, pl.ds(0, 32 * (2 ** (h - 1) - 1))], hd_sem)
        fin.wait_send()
        pl.when(y == 7)(lambda: sent(top, hs_sem.at[0]))
        pl.when(y != 7)(lambda: sent(low.at[pl.ds(2, 6)], hs_sem.at[0]))
        for h in range(2, TOP + 1):
            cond, near, far = route(h)
            count = 2 if far is None else 4
            when(cond, lambda: sent(s_f.at[pl.ds(0, count)], xs_sem.at[h]))
        finish()

    @pl.when(core == 0)
    def _():
        peer = y * 2 + 1
        mine = [
            remote(s_t.at[1], r_t.at[1], own_sem.at[0], rt_sem.at[1], row, peer),
            remote(s_f.at[1], r_f.at[1], own_sem.at[1], rf_sem.at[1], row, peer),
            remote(vasc.at[3], t_pq.at[1], own_sem.at[2], rpq_sem.at[1], row, peer),
        ]
        for c in mine:
            c.start()
        loads[2].wait()
        loads[3].wait()
        more = [
            remote(vdesc.at[3], t_sw.at[1], own_sem.at[3], rsw_sem.at[1], row, peer),
            remote(vcp.at[1, 1], t_k.at[1, 0], own_sem.at[4], rk_sem.at[1], row, peer),
            remote(vcp.at[1, 2], t_k.at[1, 1], own_sem.at[5], rk_sem.at[1], row, peer),
        ]
        for c in more:
            c.start()
        mine += more

        def low_copies(h):
            size = 2 ** (h - 1)
            base = y - y % size
            for i in range(size):
                yield table_copies(low, lows_sem, h, row, (base + i) * 2 + 1, i // (size // 2))

        def low_rest():
            arrived(low.at[pl.ds(2, 2)], low_sem.at[1])
            arrived(low.at[pl.ds(4, 4)], low_sem.at[2])
            for h in (2, 3, 4):
                @pl.when(y % 2 ** (h - 1) == 2 ** (h - 2) - 1)
                def _():
                    for k in (2, 1):
                        for c in low_copies(h):
                            for d in c[k]():
                                d.start()

        parts = (pl.ds(0, 2), pl.ds(2, 2), pl.ds(4, 4))

        def ring_copy(k, j):
            return remote(
                top.at[parts[k]], top.at[parts[k]], y_sem.at[k], top_sem.at[k], row, j * 2
            )

        def holds(h):
            return x % 2 == 0 if h == 5 else x == 1 if h == 6 else x == 3

        def along_x(h, k, src, side):
            first = x if h == 5 else 0
            for i in range(2 if h == 5 else 4):
                half = {5: i, 6: i // 2}.get(h, side)
                for d in table_copies(src, tab_sem.at[h - 5], h, z * N_X + first + i, peer, half)[k]():
                    yield d

        def along_z(h, k, places=None):
            size = 2 ** (h - 6)
            slots = mid.at[h - 7]
            for i in places or range(min(size, 4)):
                if i == size // 2 - 1:
                    continue
                to = ((z - z % size + i) * N_X + 3, y * 2)
                sems = (tab_sem.at[h - 5, k], mid_sem.at[h - 7, k])
                if k < 2:
                    yield remote(top.at[parts[k]], slots.at[parts[k]], *sems, *to)
                else:
                    side = i // (size // 2)
                    yield remote(top.at[4 + side], slots.at[4], *sems, *to)
                    yield remote(top.at[7 - side], slots.at[5], *sems, *to)

        def upper(k, heights):
            here = (row % 8 != 7) if heights[0] == 5 else (row % 8 == 7) & (row != 31)

            @pl.when(here)
            def _():
                arrived(top.at[parts[k]], top_sem.at[k], f"wait_top{k}")

                @pl.when(y == 7)
                def _():
                    for j in (2, 4, 0, 6):
                        ring_copy(k, j).start()

                @pl.when(relay == 1)
                def _():
                    ring_copy(k, jnp.where(y == 6, 5, y + 1)).start()

                for h in heights:
                    @pl.when(holds(h) if h < 7 else holds(h) & (z == keeper(h)))
                    def _():
                        if h >= 7:
                            for d in along_z(h, k):
                                d.start()
                        for d in along_x(h, k, top, 0):
                            d.start()

        def onward(k, h):
            @pl.when((x == 3) & (z != keeper(h)))
            def _():
                part = pl.ds(4, 2) if k == 2 else parts[k]
                arrived(mid.at[h - 7, part], mid_sem.at[h - 7, k], f"wait_mid{h}")
                for d in along_x(h, k, mid.at[h - 7], None):
                    d.start()

        def first_tables():
            upper(0, (5, 6, 7))
            upper(2, (8, 9))

        def local_work():
            loads[5].wait()
            loads[6].wait()
            for i in range(2):
                for r in range(4):
                    dense(i, r)
            loads[4].wait()
            arrived(r_f.at[1], rf_sem.at[1])
            for i in range(2):
                side_terms(i, vcp[1, 0], vcp[1, 3])

        @pl.when(y == 7)
        def _():
            first_tables()

        with jax.named_scope("local"):
            local_work()

        @pl.when(y != 7)
        def _():
            first_tables()

        with jax.named_scope("go"):
            pl.semaphore_wait(go_sem, 1)
        pl.when(y != 7)(low_rest)
        onward(0, 7)

        @pl.when(row == 15)
        def _():
            pl.semaphore_wait(mrdy_sem, 4)
            for d in along_z(9, 2, range(4, 8)):
                d.start()

        onward(2, 8)
        onward(2, 9)
        upper(2, (5, 6, 7))
        onward(2, 7)
        upper(1, (5, 6, 7))
        onward(1, 7)

        arrived(r_fin, fr_sem, "wait_fin")
        prepare(r_fin[2], r_fin[0], r_fin[1])

        for c in mine:
            c.wait_send()

        @pl.when(y != 7)
        def _():
            for h in (2, 3, 4):
                @pl.when(y % 2 ** (h - 1) == 2 ** (h - 2) - 1)
                def _():
                    for k in (1, 2):
                        sent(acc.at[0, pl.ds(0, 32 * 2 ** (h - 1))], lows_sem.at[k])

        def drained(k, heights):
            here = (row % 8 != 7) if heights[0] == 5 else (row % 8 == 7) & (row != 31)

            @pl.when(here)
            def _():
                @pl.when(y == 7)
                def _():
                    sent(acc.at[0, pl.ds(0, 32 * 4 * (2 if k == 2 else 1))], y_sem.at[k])

                @pl.when(relay == 1)
                def _():
                    sent(acc.at[0, pl.ds(0, 32 * (2 if k == 2 else 1))], y_sem.at[k])

            for h in heights:
                if h < 7:
                    @pl.when(holds(h))
                    def _():
                        sent(acc.at[0, pl.ds(0, 32 * (2 if h == 5 else 4))], tab_sem.at[h - 5, k])
                    continue

                @pl.when((x == 3) & (z == keeper(h)))
                def _():
                    sent(acc.at[0, pl.ds(0, 32 * (4 + 2 ** (h - 6) - 1))], tab_sem.at[h - 5, k])

                @pl.when((x == 3) & (z != keeper(h)))
                def _():
                    sent(acc.at[0, pl.ds(0, 32 * 4)], tab_sem.at[h - 5, k])

        drained(0, (5, 6, 7))
        drained(1, (5, 6, 7))
        drained(2, (5, 6, 7))
        drained(2, (8, 9))

        @pl.when((y == 7) & (row % 8 == 7))
        def _():
            arrived(top.at[parts[0]], top_sem.at[0])
            arrived(top.at[parts[1]], top_sem.at[1])

        @pl.when((y == 7) & (row == 31))
        def _():
            arrived(top.at[parts[2]], top_sem.at[2])

        finish()


def shards(dense_a, dense_b, inner, outer, ascent, descent, couplings):
    dma = pltpu.SemaphoreType.DMA
    tile = (128, 128)
    return pl.pallas_call(
        kernel,
        out_shape=pltpu.VMEM((2, 512, 512), BF),
        in_specs=[pl.BlockSpec(memory_space=pltpu.HBM)] * 7,
        out_specs=pl.BlockSpec(memory_space=pltpu.VMEM),
        scratch_shapes=[
            pltpu.VMEM((2, 512, 512), BF),
            pltpu.VMEM((2, 512, 512), BF),
            pltpu.VMEM((2, 2, 512, 128), BF),
            pltpu.VMEM((2, 2, 512, 128), BF),
            pltpu.VMEM((4, 2, *tile), BF),
            pltpu.VMEM((4, 2, *tile), BF),
            pltpu.VMEM((2, 4, *tile), BF),
            pltpu.VMEM((2, 512, 512), F32),
            pltpu.VMEM((2, 512, 128), BF),
            pltpu.VMEM((2, 512, 128), BF),
            pltpu.VMEM((2, 128, 512), BF),
            pltpu.VMEM((10, *tile), BF),
            pltpu.VMEM((10, *tile), BF),
            pltpu.VMEM((10, *tile), BF),
            pltpu.VMEM((10, *tile), BF),
            pltpu.VMEM((8, 2, *tile), BF),
            pltpu.VMEM((8, 2, *tile), BF),
            pltpu.VMEM((10, 2, *tile), BF),
            pltpu.VMEM((8, *tile), BF),
            pltpu.VMEM((8, *tile), BF),
            pltpu.VMEM((3, 6, *tile), BF),
            pltpu.VMEM((3, *tile), F32),
            pltpu.VMEM((3, *tile), F32),
            dma((7,)),
            dma((10,)),
            dma((10,)),
            dma((10,)),
            dma((8,)),
            dma((8,)),
            dma((10,)),
            dma((1,)),
            dma((3,)),
            dma((3,)),
            dma((3, 3)),
            dma((3,)),
            dma((5, 3)),
            dma((3,)),
            dma((6,)),
            dma,
            dma,
            pltpu.SemaphoreType.REGULAR,
            pltpu.SemaphoreType.REGULAR,
            pltpu.SemaphoreType.REGULAR,
            dma,
        ],
        compiler_params=pltpu.CompilerParams(collective_id=0, has_side_effects=True, vmem_limit_bytes=24 * 2**20),
        name="tree",
    )(*[pltpu.with_memory_space_constraint(v, pltpu.HBM) for v in (dense_a, dense_b, inner, outer, ascent, descent, couplings)])


def solution(mesh):
    placed = (
        P(("row", "col"), None, None),
        P(("row", "col"), None, None),
        P(("row", "col"), None, None, None),
        P(("row", "col"), None, None, None),
        P(("row", "col"), None, None, None, None),
        P(("row", "col"), None, None, None, None),
        P(("row", "col"), None, None, None, None),
    )
    return jax.shard_map(
        shards, mesh=mesh, in_specs=placed, out_specs=P(("row", "col"), None, None), check_vma=False
    )
```

```python
import jax
import jax.numpy as jnp
from jax import lax
from jax.experimental import pallas as pl
from jax.experimental.pallas import tpu as pltpu
from jax.sharding import PartitionSpec as P

MESH_ID = pl.DeviceIdType.MESH
BF = jnp.bfloat16
F32 = jnp.float32
N_X = 4
N_Y = 8
N_Z = 8
GO = 3
TOP = 9


def flip1(p):
    return p + 1 - 2 * (p % 2)


def flip3(p):
    return p - p % 4 + 3 - p % 4


def halves(v):
    if v.dtype == BF:
        return (v,)
    high = v.astype(BF)
    return high, (v - high.astype(F32)).astype(BF)


def product(a, b, ca, cb):
    a, b = halves(a), halves(b)
    terms = [(i, j) for i in range(len(a)) for j in range(len(b)) if i + j < 2]
    if len(terms) == 1:
        left, right = a[0], b[0]
    else:
        left = jnp.concatenate([a[i] for i, _ in terms], ca)
        right = jnp.concatenate([b[j] for _, j in terms], cb)
    return lax.dot_general(left, right, (((ca,), (cb,)), ((), ())), preferred_element_type=F32)


def mm(a, b):
    return product(a, b, 1, 0)


def mm_t0(a, b):
    return product(a, b, 0, 0)


def mm_t1(a, b):
    return product(a, b, 1, 1)


def kernel(
    da, db, ib, ob, asc, desc, cp, out,
    va, vb, vib, vob, vasc, vdesc, vcp,
    acc, us, vw, bw, s_f, s_t, r_f, r_t,
    t_pq, t_sw, t_k, low, top, mid, s_fin, r_fin,
    ld_sem, xs_sem, rf_sem, rt_sem, rpq_sem, rsw_sem, rk_sem,
    hs_sem, low_sem, top_sem, mid_sem, y_sem, tab_sem, lows_sem, own_sem, fs_sem, fr_sem, go_sem, rdy_sem, mrdy_sem, hd_sem,
):
    row = lax.axis_index("row")
    col = lax.axis_index("col")
    z, x = row // N_X, row % N_X
    y, core = col // 2, col % 2

    def position(h):
        return y if h <= 4 else x if h <= 6 else z

    def route(h):
        p = position(h)
        if h in (2, 5, 7):
            return None, flip1(p), None
        if h == 6:
            return None, 3 - p, None
        middle = ((p + 1) // 2) % 2
        if h in (3, 8):
            near = flip3(p)
            return middle == 1, near, flip1(near)
        near = 7 - p
        return middle == 0, near, flip1(near)

    def sender(h, p):
        if h in (2, 5, 7):
            return flip1(p)
        if h == 6:
            return 3 - p
        middle = ((p + 1) // 2) % 2
        if h in (3, 8):
            return jnp.where(middle == 1, flip3(p), flip1(flip3(p)))
        return jnp.where(middle == 0, 7 - p, flip1(7 - p))

    def place(h, p, c):
        if h <= 4:
            return row, p * 2 + c
        if h <= 6:
            return z * N_X + p, y * 2 + c
        return p * N_X + x, y * 2 + c

    def keeper(h):
        size = 2 ** (h - 6)
        return z - z % size + size // 2 - 1

    loads = []
    pairs = ((ib, vib), (asc.at[0], vasc), (desc.at[0], vdesc), (cp.at[0], vcp), (ob, vob), (da, va), (db, vb))
    for i, (src, dst) in enumerate(pairs):
        loads.append(pltpu.make_async_copy(src, dst, ld_sem.at[i]))
    for i in (1, 0):
        loads[i].start()

    barrier = pltpu.get_barrier_semaphore()

    def greet(r, c):
        pl.semaphore_signal(barrier, inc=1, device_id=(r, c), device_id_type=MESH_ID)

    middle_y, middle_z = ((y + 1) // 2) % 2, ((z + 1) // 2) % 2
    low_size = jnp.where(y % 2 == 0, 2, jnp.where(y % 4 == 1, 4, 8))
    below = jnp.where(z % 2 == 0, 1, jnp.where(z % 4 == 1, 3, jnp.where(z == 3, 3, 0)))
    upper_half = z // 4
    top_size = jnp.where(x <= 2, 4, 12 + below)
    relay = jnp.where((y % 2 == 0) & (y != 4), 1, 0)

    @pl.when(core == 0)
    def _():
        greet(row, col + 1)
        pl.when(upper_half == 0)(lambda: greet(sender(TOP, z) * N_X + x, y * 2 + 1))

        for h in (7, 8, 9):
            @pl.when((x == 3) & (z != keeper(h)) & ((h < 9) | (upper_half == 0)))
            def _():
                greet(keeper(h) * N_X + 3, y * 2)

        @pl.when(row == 15)
        def _():
            for i in range(4, 8):
                greet(i * N_X + 3, y * 2)

        @pl.when(y != 7)
        def _():
            greet(row, jnp.where(y % 2 == 0, 7, jnp.where(y == 5, 6, y - 1)) * 2)

    @pl.when(core == 1)
    def _():
        greet(row, col - 1)
        for h in (2, 3, 4):
            keeps = y - y % 2 ** (h - 1) + 2 ** (h - 2) - 1
            greet(row, keeps * 2)
            pl.when(keeps != y)(lambda: greet(row, keeps * 2 + 1))
        for h in range(2, TOP):
            greet(*place(h, sender(h, position(h)), 1))
        pl.when(upper_half == 0)(lambda: greet(*place(TOP, sender(TOP, z), 1)))

        @pl.when((upper_half == 0) & (middle_z == 0))
        def _():
            for c in (0, 1):
                greet(*place(TOP, 7 - z, c))
                greet(*place(TOP, flip1(7 - z), c))

        for holder in (x - x % 2, (x - x % 2 + 2) % 4, 1, 3, 3, 3):
            greet(z * N_X + holder, y * 2)
        greet(*place(5, 3 - flip1(x), 1))

    receivers = jnp.where(
        core == 0,
        1 + jnp.where(y == 7, 4, low_size) + relay + top_size + upper_half * (1 + x // 3),
        6 + 2 + jnp.where(y == 7, 0, low_size - 1) + 2 * middle_z + upper_half * (4 * (1 - middle_z) + 1),
    )

    with jax.named_scope("load"):
        loads[1].wait()
        up = [mm(vasc[i, 0], vasc[2, 0]) for i in range(2)], [mm(vasc[i, 1], vasc[2, 1]) for i in range(2)]
        loads[0].wait()
        for c in loads[2:]:
            c.start()
    leaf = [mm_t0(vib[i, 0], vib[i, 1]) for i in range(2)]
    lifted = sum(mm(mm_t0(up[0][i], leaf[i]), up[1][i]) for i in range(2))
    s_t[1] = lifted.astype(BF)
    node = sum(mm(mm_t0(vasc[i, 0], leaf[i]), vasc[i, 1]) for i in range(2))
    s_f[1] = node.astype(BF)

    with jax.named_scope("entry"):
        pl.semaphore_wait(barrier, receivers)

    @pl.when(upper_half == 1)
    def _():
        pl.semaphore_signal(rdy_sem, inc=1, device_id=place(TOP, sender(TOP, z), 1), device_id_type=MESH_ID)

        @pl.when((core == 0) & (x == 3))
        def _():
            pl.semaphore_signal(mrdy_sem, inc=1, device_id=(15, y * 2), device_id_type=MESH_ID)

    def remote(src, dst, ssem, rsem, r, c):
        return pltpu.make_async_remote_copy(
            src_ref=src, dst_ref=dst, send_sem=ssem, recv_sem=rsem,
            device_id=(r, c), device_id_type=MESH_ID,
        )

    def arrived(dst, sem, name="wait"):
        with jax.named_scope(name):
            remote(dst, dst, xs_sem.at[0], sem, row, col).wait_recv()

    def sent(src, sem):
        remote(src, src, sem, rf_sem.at[0], row, col).wait_send()

    def dense(i, r):
        rows = pl.ds(r * 128, 128)
        acc[i, rows, :] = jnp.dot(va[i, rows, :], vb[i], preferred_element_type=F32)

    def side_terms(i, kl1, kr1):
        near_node = mm(mm(kl1, r_f[1]), kr1)
        if True:
            kl, kr = (vcp[0, 0], vcp[0, 3]) if i == 0 else (vcp[0, 1], vcp[0, 2])
            g = mm(mm(kl, leaf[1 - i]), kr)
            g = g + mm_t1(mm(vdesc[i, 0], near_node), vdesc[i, 1])
            us[i] = mm(vob[i, 0], mm(vdesc[i, 0], vdesc[2, 0])).astype(BF)
            vw[i] = mm(vob[i, 1], mm(vdesc[i, 1], vdesc[2, 1])).astype(BF)
            acc[i] += mm_t1(mm(vob[i, 0], g.astype(BF)).astype(BF), vob[i, 1])

    def prepare(g, left, right):
        for i in range(2):
            acc[i] += mm_t1(mm(us[i], g.astype(BF)).astype(BF), vw[i])
            us[i] = mm(us[i], left).astype(BF)
            bw[i] = mm_t1(right, vw[i]).astype(BF)

    def finish():
        arrived(r_f.at[TOP], rf_sem.at[TOP], "wait_f9")
        for i in range(2):
            spread = mm(us[i], r_f[TOP]).astype(BF)
            for r in range(2):
                rows = pl.ds(r * 256, 256)
                block = acc[i, rows, :] + mm(spread[r * 256:(r + 1) * 256], bw[i])
                out[i, rows, :] = block.astype(BF)

    def when(cond, f):
        if cond is None:
            f()
        else:
            pl.when(cond)(f)

    def send_f(h, p, c):
        r, cc = place(h, p, c)
        return remote(s_f.at[h], r_f.at[h], xs_sem.at[h], rf_sem.at[h], r, cc)

    def send_t(h, p):
        r, cc = place(h, p, 1)
        return remote(s_t.at[h], r_t.at[h], xs_sem.at[h], rt_sem.at[h], r, cc)

    def table_copies(src, sem, h, r, c, side):
        return (
            lambda: (remote(src.at[pl.ds(0, 2)], t_pq.at[h], sem.at[0], rpq_sem.at[h], r, c),),
            lambda: (remote(src.at[pl.ds(2, 2)], t_sw.at[h], sem.at[1], rsw_sem.at[h], r, c),),
            lambda: (
                remote(src.at[4 if side is None else 4 + side], t_k.at[h, 0], sem.at[2], rk_sem.at[h], r, c),
                remote(src.at[5 if side is None else 7 - side], t_k.at[h, 1], sem.at[2], rk_sem.at[h], r, c),
            ),
        )

    @pl.when(core == 1)
    def _():
        me_c = y * 2 + 1
        send = remote(s_f.at[1], r_f.at[1], xs_sem.at[1], rf_sem.at[1], row, me_c - 1)
        send.start()
        loads[2].wait()
        loads[3].wait()

        def hand_over(dst, sems):
            return [
                remote(vasc.at[3], dst.at[pl.ds(0, 2)], hs_sem.at[0], sems.at[0], row, me_c - 1),
                remote(vdesc.at[3], dst.at[pl.ds(2, 2)], hs_sem.at[0], sems.at[1], row, me_c - 1),
                remote(vcp.at[1], dst.at[pl.ds(4, 4)], hs_sem.at[0], sems.at[2], row, me_c - 1),
            ]

        def hand_all():
            @pl.when(y == 7)
            def _():
                for c in hand_over(top, top_sem):
                    c.start()

            @pl.when(y != 7)
            def _():
                for c in hand_over(low, low_sem)[1:]:
                    c.start()

        def ahead(h):
            size = 2 ** (h - 1)
            base = y - y % size
            order = {2: (1,), 3: (3, 0, 2), 4: (7, 0, 6, 1, 5, 2, 4)}[h]
            own = pltpu.make_async_copy(vasc.at[3], t_pq.at[h], rpq_sem.at[h])
            return own, [
                remote(vasc.at[3], t_pq.at[h], hd_sem, rpq_sem.at[h], row, (base + i) * 2 + 1) for i in order
            ]

        def spread_ahead(heights):
            for h in heights:
                @pl.when(y % 2 ** (h - 1) == 2 ** (h - 2) - 1)
                def _():
                    own, others = ahead(h)
                    for c in others:
                        c.start()
                    own.start()

        spread_ahead((2,))
        hand_all()
        down = {}

        def compose(h):
            arrived(t_k.at[h], rk_sem.at[h], f"wait_k{h}")
            left, right = t_k[h, 0], t_k[h, 1]
            if h >= 3:
                arrived(t_sw.at[h - 2], rsw_sem.at[h - 2], f"wait_sw{h - 2}")
                s, w = t_sw[h - 2, 0], t_sw[h - 2, 1]
                if h == 3:
                    down["s"], down["w"] = s, w.T
                else:
                    down["s"] = mm(down["s"], s)
                    down["w"] = mm_t0(w, down["w"])
                left = mm(down["s"], left)
                right = mm(right, down["w"])
            if h == TOP:
                return left, right
            if h != 6:
                arrived(r_f.at[h], rf_sem.at[h], f"wait_f{h}")
            g = mm(mm(left, r_f[h]), right)
            down["g"] = g if h == 2 else down["g"] + g

        def filler(h):
            if h == 2:
                loads[5].wait()
                loads[6].wait()
                for r in range(4):
                    dense(0, r)
            if h == 3:
                for r in range(4):
                    dense(1, r)
                arrived(t_k.at[1], rk_sem.at[1])
                loads[4].wait()
                side_terms(0, t_k[1, 0], t_k[1, 1])
            if h == 4:
                side_terms(1, t_k[1, 0], t_k[1, 1])
            if h == 7:
                compose(2)
                compose(3)
            if h == 8:
                compose(4)

        arrived(r_f.at[1], rf_sem.at[1])
        arrived(r_t.at[1], rt_sem.at[1], "wait_t1")
        current = lifted + r_t[1].astype(F32)
        for h in range(2, TOP + 1):
            if h == 6:
                continue
            cond, near, far = route(h)
            s_f[h] = current.astype(BF)
            if h == TOP:
                def go():
                    pl.when(upper_half == 0)(lambda: pl.semaphore_wait(rdy_sem, 4))
                    for p, c in ((near, 1), (near, 0), (far, 1), (far, 0)):
                        send_f(h, p, c).start()
                when(cond, go)
                break
            if h in (2, 7):
                arrived(t_pq.at[h - 1], rpq_sem.at[h - 1], f"wait_pq{h - 1}")
                term = mm(mm_t0(t_pq[h - 1, 0], current), t_pq[h - 1, 1])
            else:
                term = mm(mm(turned, current), t_pq[h - 1, 1])
            s_t[h] = term.astype(BF)

            def go():
                if h == 5:
                    for p, slot in ((3 - flip1(x), 0), (3 - x, 6)):
                        remote(s_t.at[5], r_t.at[slot], xs_sem.at[5], rt_sem.at[slot], *place(5, p, 1)).start()
                if far is not None:
                    send_t(h, far).start()
                send_t(h, near).start()
                if far is not None:
                    send_f(h, far, 1).start()
                send_f(h, near, 1).start()
            when(cond, go)
            if h == 2:
                spread_ahead((3, 4))
            with jax.named_scope(f"fill{h}"):
                filler(h)
            if h < TOP - 1:
                arrived(t_pq.at[h], rpq_sem.at[h], f"wait_pq{h}")
                turned = t_pq[h, 0].T
            if h == 5:
                arrived(t_pq.at[0], rpq_sem.at[0], "wait_pq0")
                turned_other = t_pq[0, 0].T
            arrived(r_t.at[h], rt_sem.at[h], f"wait_t{h}")
            current = term + r_t[h].astype(F32)
            if h == 5:
                arrived(r_t.at[6], rt_sem.at[6], "wait_t6")
                arrived(r_t.at[0], rt_sem.at[0], "wait_t0")
                other = r_t[6].astype(F32) + r_t[0].astype(F32)
                r_f[6] = other.astype(BF)
                current = mm(mm(turned, current), t_pq[5, 1]) + mm(mm(turned_other, other), t_pq[0, 1])
            if h == GO:
                pl.semaphore_signal(go_sem, inc=1, device_id=(row, me_c - 1), device_id_type=MESH_ID)
        compose(5)
        compose(6)
        compose(7)
        compose(8)
        left, right = compose(9)
        s_fin[0] = left
        s_fin[1] = right
        s_fin[2] = down["g"]
        fin = remote(s_fin, r_fin, fs_sem, fr_sem, row, me_c - 1)
        fin.start()
        prepare(down["g"], left, right)
        send.wait_send()
        for h in (2, 3, 4):
            @pl.when(y % 2 ** (h - 1) == 2 ** (h - 2) - 1)
            def _():
                sent(acc.at[0, pl.ds(0, 32 * (2 ** (h - 1) - 1))], hd_sem)
        fin.wait_send()
        pl.when(y == 7)(lambda: sent(top, hs_sem.at[0]))
        pl.when(y != 7)(lambda: sent(low.at[pl.ds(2, 6)], hs_sem.at[0]))
        for h in range(2, TOP + 1):
            cond, near, far = route(h)
            if h == 6:
                continue
            count = 2 if far is None and h != 5 else 4
            when(cond, lambda: sent(s_f.at[pl.ds(0, count)], xs_sem.at[h]))
        finish()

    @pl.when(core == 0)
    def _():
        peer = y * 2 + 1
        mine = [
            remote(s_t.at[1], r_t.at[1], own_sem.at[0], rt_sem.at[1], row, peer),
            remote(s_f.at[1], r_f.at[1], own_sem.at[1], rf_sem.at[1], row, peer),
            remote(vasc.at[3], t_pq.at[1], own_sem.at[2], rpq_sem.at[1], row, peer),
        ]
        for c in mine:
            c.start()
        loads[2].wait()
        loads[3].wait()
        more = [
            remote(vdesc.at[3], t_sw.at[1], own_sem.at[3], rsw_sem.at[1], row, peer),
            remote(vcp.at[1, 1], t_k.at[1, 0], own_sem.at[4], rk_sem.at[1], row, peer),
            remote(vcp.at[1, 2], t_k.at[1, 1], own_sem.at[5], rk_sem.at[1], row, peer),
        ]
        for c in more:
            c.start()
        mine += more

        def low_copies(h):
            size = 2 ** (h - 1)
            base = y - y % size
            for i in range(size):
                yield table_copies(low, lows_sem, h, row, (base + i) * 2 + 1, i // (size // 2))

        def low_rest():
            arrived(low.at[pl.ds(2, 2)], low_sem.at[1])
            arrived(low.at[pl.ds(4, 4)], low_sem.at[2])
            for h in (2, 3, 4):
                @pl.when(y % 2 ** (h - 1) == 2 ** (h - 2) - 1)
                def _():
                    for k in (2, 1):
                        for c in low_copies(h):
                            for d in c[k]():
                                d.start()

        parts = (pl.ds(0, 2), pl.ds(2, 2), pl.ds(4, 4))

        def ring_copy(k, j):
            return remote(
                top.at[parts[k]], top.at[parts[k]], y_sem.at[k], top_sem.at[k], row, j * 2
            )

        def holds(h):
            return x % 2 == 0 if h == 5 else x == 1 if h == 6 else x == 3

        def along_x(h, k, src, side):
            if (h, k) == (5, 0):
                for i in range(4):
                    slot = jnp.where(x // 2 == i // 2, 5, 0)
                    for d in table_copies(src, tab_sem.at[0], slot, z * N_X + i, peer, 0)[0]():
                        yield d
                return
            first = x if h == 5 else 0
            for i in range(2 if h == 5 else 4):
                half = {5: i, 6: i // 2}.get(h, side)
                for d in table_copies(src, tab_sem.at[h - 5], h, z * N_X + first + i, peer, half)[k]():
                    yield d

        def along_z(h, k, places=None):
            size = 2 ** (h - 6)
            slots = mid.at[h - 7]
            for i in places or range(min(size, 4)):
                if i == size // 2 - 1:
                    continue
                to = ((z - z % size + i) * N_X + 3, y * 2)
                sems = (tab_sem.at[h - 5, k], mid_sem.at[h - 7, k])
                if k < 2:
                    yield remote(top.at[parts[k]], slots.at[parts[k]], *sems, *to)
                else:
                    side = i // (size // 2)
                    yield remote(top.at[4 + side], slots.at[4], *sems, *to)
                    yield remote(top.at[7 - side], slots.at[5], *sems, *to)

        def upper(k, heights):
            here = (row % 8 != 7) if heights[0] == 5 else (row % 8 == 7) & (row != 31)

            @pl.when(here)
            def _():
                arrived(top.at[parts[k]], top_sem.at[k], f"wait_top{k}")

                @pl.when(y == 7)
                def _():
                    for j in (2, 4, 0, 6):
                        ring_copy(k, j).start()

                @pl.when(relay == 1)
                def _():
                    ring_copy(k, jnp.where(y == 6, 5, y + 1)).start()

                for h in heights:
                    @pl.when(holds(h) if h < 7 else holds(h) & (z == keeper(h)))
                    def _():
                        if h >= 7:
                            for d in along_z(h, k):
                                d.start()
                        for d in along_x(h, k, top, 0):
                            d.start()

        def onward(k, h):
            @pl.when((x == 3) & (z != keeper(h)))
            def _():
                part = pl.ds(4, 2) if k == 2 else parts[k]
                arrived(mid.at[h - 7, part], mid_sem.at[h - 7, k], f"wait_mid{h}")
                for d in along_x(h, k, mid.at[h - 7], None):
                    d.start()

        def first_tables():
            upper(0, (5, 6, 7))
            upper(2, (8, 9))

        def local_work():
            loads[5].wait()
            loads[6].wait()
            for i in range(2):
                for r in range(4):
                    dense(i, r)
            loads[4].wait()
            arrived(r_f.at[1], rf_sem.at[1])
            for i in range(2):
                side_terms(i, vcp[1, 0], vcp[1, 3])

        @pl.when(y == 7)
        def _():
            first_tables()

        with jax.named_scope("local"):
            local_work()

        @pl.when(y != 7)
        def _():
            first_tables()

        with jax.named_scope("go"):
            pl.semaphore_wait(go_sem, 1)
        pl.when(y != 7)(low_rest)
        onward(0, 7)

        @pl.when(row == 15)
        def _():
            pl.semaphore_wait(mrdy_sem, 4)
            for d in along_z(9, 2, range(4, 8)):
                d.start()

        onward(2, 8)
        onward(2, 9)
        upper(2, (5, 6, 7))
        onward(2, 7)
        upper(1, (5, 6, 7))
        onward(1, 7)

        arrived(r_fin, fr_sem, "wait_fin")
        prepare(r_fin[2], r_fin[0], r_fin[1])

        for c in mine:
            c.wait_send()

        @pl.when(y != 7)
        def _():
            for h in (2, 3, 4):
                @pl.when(y % 2 ** (h - 1) == 2 ** (h - 2) - 1)
                def _():
                    for k in (1, 2):
                        sent(acc.at[0, pl.ds(0, 32 * 2 ** (h - 1))], lows_sem.at[k])

        def drained(k, heights):
            here = (row % 8 != 7) if heights[0] == 5 else (row % 8 == 7) & (row != 31)

            @pl.when(here)
            def _():
                @pl.when(y == 7)
                def _():
                    sent(acc.at[0, pl.ds(0, 32 * 4 * (2 if k == 2 else 1))], y_sem.at[k])

                @pl.when(relay == 1)
                def _():
                    sent(acc.at[0, pl.ds(0, 32 * (2 if k == 2 else 1))], y_sem.at[k])

            for h in heights:
                if h < 7:
                    @pl.when(holds(h))
                    def _():
                        sent(acc.at[0, pl.ds(0, 32 * (2 if h == 5 and k else 4))], tab_sem.at[h - 5, k])
                    continue

                @pl.when((x == 3) & (z == keeper(h)))
                def _():
                    sent(acc.at[0, pl.ds(0, 32 * (4 + 2 ** (h - 6) - 1))], tab_sem.at[h - 5, k])

                @pl.when((x == 3) & (z != keeper(h)))
                def _():
                    sent(acc.at[0, pl.ds(0, 32 * 4)], tab_sem.at[h - 5, k])

        drained(0, (5, 6, 7))
        drained(1, (5, 6, 7))
        drained(2, (5, 6, 7))
        drained(2, (8, 9))

        @pl.when((y == 7) & (row % 8 == 7))
        def _():
            arrived(top.at[parts[0]], top_sem.at[0])
            arrived(top.at[parts[1]], top_sem.at[1])

        @pl.when((y == 7) & (row == 31))
        def _():
            arrived(top.at[parts[2]], top_sem.at[2])

        finish()


def shards(dense_a, dense_b, inner, outer, ascent, descent, couplings):
    dma = pltpu.SemaphoreType.DMA
    tile = (128, 128)
    return pl.pallas_call(
        kernel,
        out_shape=pltpu.VMEM((2, 512, 512), BF),
        in_specs=[pl.BlockSpec(memory_space=pltpu.HBM)] * 7,
        out_specs=pl.BlockSpec(memory_space=pltpu.VMEM),
        scratch_shapes=[
            pltpu.VMEM((2, 512, 512), BF),
            pltpu.VMEM((2, 512, 512), BF),
            pltpu.VMEM((2, 2, 512, 128), BF),
            pltpu.VMEM((2, 2, 512, 128), BF),
            pltpu.VMEM((4, 2, *tile), BF),
            pltpu.VMEM((4, 2, *tile), BF),
            pltpu.VMEM((2, 4, *tile), BF),
            pltpu.VMEM((2, 512, 512), F32),
            pltpu.VMEM((2, 512, 128), BF),
            pltpu.VMEM((2, 512, 128), BF),
            pltpu.VMEM((2, 128, 512), BF),
            pltpu.VMEM((10, *tile), BF),
            pltpu.VMEM((10, *tile), BF),
            pltpu.VMEM((10, *tile), BF),
            pltpu.VMEM((10, *tile), BF),
            pltpu.VMEM((8, 2, *tile), BF),
            pltpu.VMEM((8, 2, *tile), BF),
            pltpu.VMEM((10, 2, *tile), BF),
            pltpu.VMEM((8, *tile), BF),
            pltpu.VMEM((8, *tile), BF),
            pltpu.VMEM((3, 6, *tile), BF),
            pltpu.VMEM((3, *tile), F32),
            pltpu.VMEM((3, *tile), F32),
            dma((7,)),
            dma((10,)),
            dma((10,)),
            dma((10,)),
            dma((8,)),
            dma((8,)),
            dma((10,)),
            dma((1,)),
            dma((3,)),
            dma((3,)),
            dma((3, 3)),
            dma((3,)),
            dma((5, 3)),
            dma((3,)),
            dma((6,)),
            dma,
            dma,
            pltpu.SemaphoreType.REGULAR,
            pltpu.SemaphoreType.REGULAR,
            pltpu.SemaphoreType.REGULAR,
            dma,
        ],
        compiler_params=pltpu.CompilerParams(collective_id=0, has_side_effects=True, vmem_limit_bytes=24 * 2**20),
        name="tree",
    )(*[pltpu.with_memory_space_constraint(v, pltpu.HBM) for v in (dense_a, dense_b, inner, outer, ascent, descent, couplings)])


def solution(mesh):
    placed = (
        P(("row", "col"), None, None),
        P(("row", "col"), None, None),
        P(("row", "col"), None, None, None),
        P(("row", "col"), None, None, None),
        P(("row", "col"), None, None, None, None),
        P(("row", "col"), None, None, None, None),
        P(("row", "col"), None, None, None, None),
    )
    return jax.shard_map(
        shards, mesh=mesh, in_specs=placed, out_specs=P(("row", "col"), None, None), check_vma=False
    )
```

```python
import jax
import jax.numpy as jnp
from jax import lax
from jax.experimental import pallas as pl
from jax.experimental.pallas import tpu as pltpu
from jax.sharding import PartitionSpec as P

MESH_ID = pl.DeviceIdType.MESH
BF = jnp.bfloat16
F32 = jnp.float32
N_X = 4
N_Y = 8
N_Z = 8
GO = 3
TOP = 9


def flip1(p):
    return p + 1 - 2 * (p % 2)


def flip3(p):
    return p - p % 4 + 3 - p % 4


def halves(v):
    if v.dtype == BF:
        return (v,)
    high = v.astype(BF)
    return high, (v - high.astype(F32)).astype(BF)


def product(a, b, ca, cb):
    a, b = halves(a), halves(b)
    terms = [(i, j) for i in range(len(a)) for j in range(len(b)) if i + j < 2]
    if len(terms) == 1:
        left, right = a[0], b[0]
    else:
        left = jnp.concatenate([a[i] for i, _ in terms], ca)
        right = jnp.concatenate([b[j] for _, j in terms], cb)
    return lax.dot_general(left, right, (((ca,), (cb,)), ((), ())), preferred_element_type=F32)


def mm(a, b):
    return product(a, b, 1, 0)


def mm_t0(a, b):
    return product(a, b, 0, 0)


def mm_t1(a, b):
    return product(a, b, 1, 1)


def kernel(
    da, db, ib, ob, asc, desc, cp, out,
    va, vb, vib, vob, vasc, vdesc, vcp,
    acc, us, vw, bw, s_f, s_t, r_f, r_t,
    t_pq, t_sw, t_k, low, top, mid, s_fin, r_fin,
    ld_sem, xs_sem, rf_sem, rt_sem, rpq_sem, rsw_sem, rk_sem,
    hs_sem, low_sem, top_sem, mid_sem, y_sem, tab_sem, lows_sem, own_sem, fs_sem, fr_sem, go_sem, rdy_sem, mrdy_sem, hd_sem,
):
    row = lax.axis_index("row")
    col = lax.axis_index("col")
    z, x = row // N_X, row % N_X
    y, core = col // 2, col % 2

    def position(h):
        return y if h <= 4 else x if h <= 6 else z

    def route(h):
        p = position(h)
        if h in (2, 5, 7):
            return None, flip1(p), None
        if h == 6:
            return None, 3 - p, None
        middle = ((p + 1) // 2) % 2
        if h in (3, 8):
            near = flip3(p)
            return middle == 1, near, flip1(near)
        near = 7 - p
        return middle == 0, near, flip1(near)

    def sender(h, p):
        if h in (2, 5, 7):
            return flip1(p)
        if h == 6:
            return 3 - p
        middle = ((p + 1) // 2) % 2
        if h in (3, 8):
            return jnp.where(middle == 1, flip3(p), flip1(flip3(p)))
        return jnp.where(middle == 0, 7 - p, flip1(7 - p))

    def place(h, p, c):
        if h <= 4:
            return row, p * 2 + c
        if h <= 6:
            return z * N_X + p, y * 2 + c
        return p * N_X + x, y * 2 + c

    def keeper(h):
        size = 2 ** (h - 6)
        return z - z % size + size // 2 - 1

    loads = []
    pairs = ((ib, vib), (asc.at[0], vasc), (desc.at[0], vdesc), (cp.at[0], vcp), (ob, vob), (da, va), (db, vb))
    for i, (src, dst) in enumerate(pairs):
        loads.append(pltpu.make_async_copy(src, dst, ld_sem.at[i]))
    leaf_loads = [
        pltpu.make_async_copy(ib.at[i, j], vib.at[i, j], ld_sem.at[7 + 2 * i + j]) for i in range(2) for j in range(2)
    ]
    for c in (loads[1], *leaf_loads):
        c.start()

    barrier = pltpu.get_barrier_semaphore()

    def greet(r, c):
        pl.semaphore_signal(barrier, inc=1, device_id=(r, c), device_id_type=MESH_ID)

    middle_y, middle_z = ((y + 1) // 2) % 2, ((z + 1) // 2) % 2
    low_size = jnp.where(y % 2 == 0, 2, jnp.where(y % 4 == 1, 4, 8))
    below = jnp.where(z % 2 == 0, 1, jnp.where(z % 4 == 1, 3, jnp.where(z == 3, 3, 0)))
    upper_half = z // 4
    top_size = jnp.where(x <= 2, 4, 12 + below)
    relay = jnp.where((y % 2 == 0) & (y != 4), 1, 0)

    @pl.when(core == 0)
    def _():
        greet(row, col + 1)
        pl.when(upper_half == 0)(lambda: greet(sender(TOP, z) * N_X + x, y * 2 + 1))

        for h in (7, 8, 9):
            @pl.when((x == 3) & (z != keeper(h)) & ((h < 9) | (upper_half == 0)))
            def _():
                greet(keeper(h) * N_X + 3, y * 2)

        @pl.when(row == 15)
        def _():
            for i in range(4, 8):
                greet(i * N_X + 3, y * 2)

        @pl.when(y != 7)
        def _():
            greet(row, jnp.where(y % 2 == 0, 7, jnp.where(y == 5, 6, y - 1)) * 2)

    @pl.when(core == 1)
    def _():
        greet(row, col - 1)
        for h in (2, 3, 4):
            keeps = y - y % 2 ** (h - 1) + 2 ** (h - 2) - 1
            greet(row, keeps * 2)
            pl.when(keeps != y)(lambda: greet(row, keeps * 2 + 1))
        for h in range(2, TOP):
            greet(*place(h, sender(h, position(h)), 1))
        pl.when(upper_half == 0)(lambda: greet(*place(TOP, sender(TOP, z), 1)))

        @pl.when((upper_half == 0) & (middle_z == 0))
        def _():
            for c in (0, 1):
                greet(*place(TOP, 7 - z, c))
                greet(*place(TOP, flip1(7 - z), c))

        for holder in (x - x % 2, (x - x % 2 + 2) % 4, 1, 3, 3, 3):
            greet(z * N_X + holder, y * 2)
        greet(*place(5, 3 - flip1(x), 1))

    receivers = jnp.where(
        core == 0,
        1 + jnp.where(y == 7, 4, low_size) + relay + top_size + upper_half * (1 + x // 3),
        6 + 2 + jnp.where(y == 7, 0, low_size - 1) + 2 * middle_z + upper_half * (4 * (1 - middle_z) + 1),
    )

    with jax.named_scope("load"):
        loads[1].wait()
        up = [mm(vasc[i, 0], vasc[2, 0]) for i in range(2)], [mm(vasc[i, 1], vasc[2, 1]) for i in range(2)]
        for c in leaf_loads:
            c.wait()
        for c in loads[2:]:
            c.start()
    leaf = [mm_t0(vib[i, 0], vib[i, 1]) for i in range(2)]
    lifted = sum(mm(mm_t0(up[0][i], leaf[i]), up[1][i]) for i in range(2))
    s_t[1] = lifted.astype(BF)
    node = sum(mm(mm_t0(vasc[i, 0], leaf[i]), vasc[i, 1]) for i in range(2))
    s_f[1] = node.astype(BF)

    with jax.named_scope("entry"):
        pl.semaphore_wait(barrier, receivers)

    @pl.when(upper_half == 1)
    def _():
        pl.semaphore_signal(rdy_sem, inc=1, device_id=place(TOP, sender(TOP, z), 1), device_id_type=MESH_ID)

        @pl.when((core == 0) & (x == 3))
        def _():
            pl.semaphore_signal(mrdy_sem, inc=1, device_id=(15, y * 2), device_id_type=MESH_ID)

    def remote(src, dst, ssem, rsem, r, c):
        return pltpu.make_async_remote_copy(
            src_ref=src, dst_ref=dst, send_sem=ssem, recv_sem=rsem,
            device_id=(r, c), device_id_type=MESH_ID,
        )

    def arrived(dst, sem, name="wait"):
        with jax.named_scope(name):
            remote(dst, dst, xs_sem.at[0], sem, row, col).wait_recv()

    def sent(src, sem):
        remote(src, src, sem, rf_sem.at[0], row, col).wait_send()

    def dense(i, r):
        rows = pl.ds(r * 128, 128)
        acc[i, rows, :] = jnp.dot(va[i, rows, :], vb[i], preferred_element_type=F32)

    def side_terms(i, kl1, kr1):
        near_node = mm(mm(kl1, r_f[1]), kr1)
        if True:
            kl, kr = (vcp[0, 0], vcp[0, 3]) if i == 0 else (vcp[0, 1], vcp[0, 2])
            g = mm(mm(kl, leaf[1 - i]), kr)
            g = g + mm_t1(mm(vdesc[i, 0], near_node), vdesc[i, 1])
            us[i] = mm(vob[i, 0], mm(vdesc[i, 0], vdesc[2, 0])).astype(BF)
            vw[i] = mm(vob[i, 1], mm(vdesc[i, 1], vdesc[2, 1])).astype(BF)
            acc[i] += mm_t1(mm(vob[i, 0], g.astype(BF)).astype(BF), vob[i, 1])

    def prepare(g, left, right):
        for i in range(2):
            acc[i] += mm_t1(mm(us[i], g.astype(BF)).astype(BF), vw[i])
            us[i] = mm(us[i], left).astype(BF)
            bw[i] = mm_t1(right, vw[i]).astype(BF)

    def finish():
        arrived(r_f.at[TOP], rf_sem.at[TOP], "wait_f9")
        for i in range(2):
            spread = mm(us[i], r_f[TOP]).astype(BF)
            for r in range(2):
                rows = pl.ds(r * 256, 256)
                block = acc[i, rows, :] + mm(spread[r * 256:(r + 1) * 256], bw[i])
                out[i, rows, :] = block.astype(BF)

    def when(cond, f):
        if cond is None:
            f()
        else:
            pl.when(cond)(f)

    def send_f(h, p, c):
        r, cc = place(h, p, c)
        return remote(s_f.at[h], r_f.at[h], xs_sem.at[h], rf_sem.at[h], r, cc)

    def send_t(h, p):
        r, cc = place(h, p, 1)
        return remote(s_t.at[h], r_t.at[h], xs_sem.at[h], rt_sem.at[h], r, cc)

    def table_copies(src, sem, h, r, c, side):
        return (
            lambda: (remote(src.at[pl.ds(0, 2)], t_pq.at[h], sem.at[0], rpq_sem.at[h], r, c),),
            lambda: (remote(src.at[pl.ds(2, 2)], t_sw.at[h], sem.at[1], rsw_sem.at[h], r, c),),
            lambda: (
                remote(src.at[4 if side is None else 4 + side], t_k.at[h, 0], sem.at[2], rk_sem.at[h], r, c),
                remote(src.at[5 if side is None else 7 - side], t_k.at[h, 1], sem.at[2], rk_sem.at[h], r, c),
            ),
        )

    @pl.when(core == 1)
    def _():
        me_c = y * 2 + 1
        send = remote(s_f.at[1], r_f.at[1], xs_sem.at[1], rf_sem.at[1], row, me_c - 1)
        send.start()
        loads[2].wait()
        loads[3].wait()

        def hand_over(dst, sems):
            return [
                remote(vasc.at[3], dst.at[pl.ds(0, 2)], hs_sem.at[0], sems.at[0], row, me_c - 1),
                remote(vdesc.at[3], dst.at[pl.ds(2, 2)], hs_sem.at[0], sems.at[1], row, me_c - 1),
                remote(vcp.at[1], dst.at[pl.ds(4, 4)], hs_sem.at[0], sems.at[2], row, me_c - 1),
            ]

        def hand_all():
            @pl.when(y == 7)
            def _():
                for c in hand_over(top, top_sem):
                    c.start()

            @pl.when(y != 7)
            def _():
                for c in hand_over(low, low_sem)[1:]:
                    c.start()

        def ahead(h):
            size = 2 ** (h - 1)
            base = y - y % size
            order = {2: (1,), 3: (3, 0, 2), 4: (7, 0, 6, 1, 5, 2, 4)}[h]
            own = pltpu.make_async_copy(vasc.at[3], t_pq.at[h], rpq_sem.at[h])
            return own, [
                remote(vasc.at[3], t_pq.at[h], hd_sem, rpq_sem.at[h], row, (base + i) * 2 + 1) for i in order
            ]

        def spread_ahead(heights):
            for h in heights:
                @pl.when(y % 2 ** (h - 1) == 2 ** (h - 2) - 1)
                def _():
                    own, others = ahead(h)
                    for c in others:
                        c.start()
                    own.start()

        spread_ahead((2,))
        hand_all()
        down = {}

        def compose(h):
            arrived(t_k.at[h], rk_sem.at[h], f"wait_k{h}")
            left, right = t_k[h, 0], t_k[h, 1]
            if h >= 3:
                arrived(t_sw.at[h - 2], rsw_sem.at[h - 2], f"wait_sw{h - 2}")
                s, w = t_sw[h - 2, 0], t_sw[h - 2, 1]
                if h == 3:
                    down["s"], down["w"] = s, w.T
                else:
                    down["s"] = mm(down["s"], s)
                    down["w"] = mm_t0(w, down["w"])
                left = mm(down["s"], left)
                right = mm(right, down["w"])
            if h == TOP:
                return left, right
            if h != 6:
                arrived(r_f.at[h], rf_sem.at[h], f"wait_f{h}")
            g = mm(mm(left, r_f[h]), right)
            down["g"] = g if h == 2 else down["g"] + g

        def filler(h):
            if h == 2:
                loads[5].wait()
                loads[6].wait()
                for r in range(4):
                    dense(0, r)
            if h == 3:
                for r in range(4):
                    dense(1, r)
                arrived(t_k.at[1], rk_sem.at[1])
                loads[4].wait()
                side_terms(0, t_k[1, 0], t_k[1, 1])
            if h == 4:
                side_terms(1, t_k[1, 0], t_k[1, 1])
            if h == 7:
                compose(2)
                compose(3)
            if h == 8:
                compose(4)

        arrived(r_f.at[1], rf_sem.at[1])
        arrived(r_t.at[1], rt_sem.at[1], "wait_t1")
        current = lifted + r_t[1].astype(F32)
        for h in range(2, TOP + 1):
            if h == 6:
                continue
            cond, near, far = route(h)
            s_f[h] = current.astype(BF)
            if h == TOP:
                def go():
                    pl.when(upper_half == 0)(lambda: pl.semaphore_wait(rdy_sem, 4))
                    for p, c in ((near, 1), (near, 0), (far, 1), (far, 0)):
                        send_f(h, p, c).start()
                when(cond, go)
                break
            if h in (2, 7):
                arrived(t_pq.at[h - 1], rpq_sem.at[h - 1], f"wait_pq{h - 1}")
                term = mm(mm_t0(t_pq[h - 1, 0], current), t_pq[h - 1, 1])
            else:
                term = mm(mm(turned, current), t_pq[h - 1, 1])
            s_t[h] = term.astype(BF)

            def go():
                if h == 5:
                    for p, slot in ((3 - flip1(x), 0), (3 - x, 6)):
                        remote(s_t.at[5], r_t.at[slot], xs_sem.at[5], rt_sem.at[slot], *place(5, p, 1)).start()
                if far is not None:
                    send_t(h, far).start()
                send_t(h, near).start()
                if far is not None:
                    send_f(h, far, 1).start()
                send_f(h, near, 1).start()
            when(cond, go)
            if h == 2:
                spread_ahead((3, 4))
            with jax.named_scope(f"fill{h}"):
                filler(h)
            if h < TOP - 1:
                arrived(t_pq.at[h], rpq_sem.at[h], f"wait_pq{h}")
                turned = t_pq[h, 0].T
            if h == 5:
                arrived(t_pq.at[0], rpq_sem.at[0], "wait_pq0")
                turned_other = t_pq[0, 0].T
            arrived(r_t.at[h], rt_sem.at[h], f"wait_t{h}")
            current = term + r_t[h].astype(F32)
            if h == 5:
                arrived(r_t.at[6], rt_sem.at[6], "wait_t6")
                arrived(r_t.at[0], rt_sem.at[0], "wait_t0")
                other = r_t[6].astype(F32) + r_t[0].astype(F32)
                r_f[6] = other.astype(BF)
                current = mm(mm(turned, current), t_pq[5, 1]) + mm(mm(turned_other, other), t_pq[0, 1])
            if h == GO:
                pl.semaphore_signal(go_sem, inc=1, device_id=(row, me_c - 1), device_id_type=MESH_ID)
        compose(5)
        compose(6)
        compose(7)
        compose(8)
        left, right = compose(9)
        s_fin[0] = left
        s_fin[1] = right
        s_fin[2] = down["g"]
        fin = remote(s_fin, r_fin, fs_sem, fr_sem, row, me_c - 1)
        fin.start()
        prepare(down["g"], left, right)
        send.wait_send()
        for h in (2, 3, 4):
            @pl.when(y % 2 ** (h - 1) == 2 ** (h - 2) - 1)
            def _():
                sent(acc.at[0, pl.ds(0, 32 * (2 ** (h - 1) - 1))], hd_sem)
        fin.wait_send()
        pl.when(y == 7)(lambda: sent(top, hs_sem.at[0]))
        pl.when(y != 7)(lambda: sent(low.at[pl.ds(2, 6)], hs_sem.at[0]))
        for h in range(2, TOP + 1):
            cond, near, far = route(h)
            if h == 6:
                continue
            count = 2 if far is None and h != 5 else 4
            when(cond, lambda: sent(s_f.at[pl.ds(0, count)], xs_sem.at[h]))
        finish()

    @pl.when(core == 0)
    def _():
        peer = y * 2 + 1
        mine = [
            remote(s_t.at[1], r_t.at[1], own_sem.at[0], rt_sem.at[1], row, peer),
            remote(s_f.at[1], r_f.at[1], own_sem.at[1], rf_sem.at[1], row, peer),
            remote(vasc.at[3], t_pq.at[1], own_sem.at[2], rpq_sem.at[1], row, peer),
        ]
        for c in mine:
            c.start()
        loads[2].wait()
        loads[3].wait()
        more = [
            remote(vdesc.at[3], t_sw.at[1], own_sem.at[3], rsw_sem.at[1], row, peer),
            remote(vcp.at[1, 1], t_k.at[1, 0], own_sem.at[4], rk_sem.at[1], row, peer),
            remote(vcp.at[1, 2], t_k.at[1, 1], own_sem.at[5], rk_sem.at[1], row, peer),
        ]
        for c in more:
            c.start()
        mine += more

        def low_copies(h):
            size = 2 ** (h - 1)
            base = y - y % size
            for i in range(size):
                yield table_copies(low, lows_sem, h, row, (base + i) * 2 + 1, i // (size // 2))

        def low_rest():
            arrived(low.at[pl.ds(2, 2)], low_sem.at[1])
            arrived(low.at[pl.ds(4, 4)], low_sem.at[2])
            for h in (2, 3, 4):
                @pl.when(y % 2 ** (h - 1) == 2 ** (h - 2) - 1)
                def _():
                    for k in (2, 1):
                        for c in low_copies(h):
                            for d in c[k]():
                                d.start()

        parts = (pl.ds(0, 2), pl.ds(2, 2), pl.ds(4, 4))

        def ring_copy(k, j):
            return remote(
                top.at[parts[k]], top.at[parts[k]], y_sem.at[k], top_sem.at[k], row, j * 2
            )

        def holds(h):
            return x % 2 == 0 if h == 5 else x == 1 if h == 6 else x == 3

        def along_x(h, k, src, side):
            if (h, k) == (5, 0):
                for i in range(4):
                    slot = jnp.where(x // 2 == i // 2, 5, 0)
                    for d in table_copies(src, tab_sem.at[0], slot, z * N_X + i, peer, 0)[0]():
                        yield d
                return
            first = x if h == 5 else 0
            for i in range(2 if h == 5 else 4):
                half = {5: i, 6: i // 2}.get(h, side)
                for d in table_copies(src, tab_sem.at[h - 5], h, z * N_X + first + i, peer, half)[k]():
                    yield d

        def along_z(h, k, places=None):
            size = 2 ** (h - 6)
            slots = mid.at[h - 7]
            for i in places or range(min(size, 4)):
                if i == size // 2 - 1:
                    continue
                to = ((z - z % size + i) * N_X + 3, y * 2)
                sems = (tab_sem.at[h - 5, k], mid_sem.at[h - 7, k])
                if k < 2:
                    yield remote(top.at[parts[k]], slots.at[parts[k]], *sems, *to)
                else:
                    side = i // (size // 2)
                    yield remote(top.at[4 + side], slots.at[4], *sems, *to)
                    yield remote(top.at[7 - side], slots.at[5], *sems, *to)

        def upper(k, heights):
            here = (row % 8 != 7) if heights[0] == 5 else (row % 8 == 7) & (row != 31)

            @pl.when(here)
            def _():
                arrived(top.at[parts[k]], top_sem.at[k], f"wait_top{k}")

                @pl.when(y == 7)
                def _():
                    for j in (2, 4, 0, 6):
                        ring_copy(k, j).start()

                @pl.when(relay == 1)
                def _():
                    ring_copy(k, jnp.where(y == 6, 5, y + 1)).start()

                for h in heights:
                    @pl.when(holds(h) if h < 7 else holds(h) & (z == keeper(h)))
                    def _():
                        if h >= 7:
                            for d in along_z(h, k):
                                d.start()
                        for d in along_x(h, k, top, 0):
                            d.start()

        def onward(k, h):
            @pl.when((x == 3) & (z != keeper(h)))
            def _():
                part = pl.ds(4, 2) if k == 2 else parts[k]
                arrived(mid.at[h - 7, part], mid_sem.at[h - 7, k], f"wait_mid{h}")
                for d in along_x(h, k, mid.at[h - 7], None):
                    d.start()

        def first_tables():
            upper(0, (5, 6, 7))
            upper(2, (8, 9))

        def local_work():
            loads[5].wait()
            loads[6].wait()
            for i in range(2):
                for r in range(4):
                    dense(i, r)
            loads[4].wait()
            arrived(r_f.at[1], rf_sem.at[1])
            for i in range(2):
                side_terms(i, vcp[1, 0], vcp[1, 3])

        @pl.when(y == 7)
        def _():
            first_tables()

        with jax.named_scope("local"):
            local_work()

        @pl.when(y != 7)
        def _():
            first_tables()

        with jax.named_scope("go"):
            pl.semaphore_wait(go_sem, 1)
        pl.when(y != 7)(low_rest)
        onward(0, 7)

        @pl.when(row == 15)
        def _():
            pl.semaphore_wait(mrdy_sem, 4)
            for d in along_z(9, 2, range(4, 8)):
                d.start()

        onward(2, 8)
        onward(2, 9)
        upper(2, (5, 6, 7))
        onward(2, 7)
        upper(1, (5, 6, 7))
        onward(1, 7)

        arrived(r_fin, fr_sem, "wait_fin")
        prepare(r_fin[2], r_fin[0], r_fin[1])

        for c in mine:
            c.wait_send()

        @pl.when(y != 7)
        def _():
            for h in (2, 3, 4):
                @pl.when(y % 2 ** (h - 1) == 2 ** (h - 2) - 1)
                def _():
                    for k in (1, 2):
                        sent(acc.at[0, pl.ds(0, 32 * 2 ** (h - 1))], lows_sem.at[k])

        def drained(k, heights):
            here = (row % 8 != 7) if heights[0] == 5 else (row % 8 == 7) & (row != 31)

            @pl.when(here)
            def _():
                @pl.when(y == 7)
                def _():
                    sent(acc.at[0, pl.ds(0, 32 * 4 * (2 if k == 2 else 1))], y_sem.at[k])

                @pl.when(relay == 1)
                def _():
                    sent(acc.at[0, pl.ds(0, 32 * (2 if k == 2 else 1))], y_sem.at[k])

            for h in heights:
                if h < 7:
                    @pl.when(holds(h))
                    def _():
                        sent(acc.at[0, pl.ds(0, 32 * (2 if h == 5 and k else 4))], tab_sem.at[h - 5, k])
                    continue

                @pl.when((x == 3) & (z == keeper(h)))
                def _():
                    sent(acc.at[0, pl.ds(0, 32 * (4 + 2 ** (h - 6) - 1))], tab_sem.at[h - 5, k])

                @pl.when((x == 3) & (z != keeper(h)))
                def _():
                    sent(acc.at[0, pl.ds(0, 32 * 4)], tab_sem.at[h - 5, k])

        drained(0, (5, 6, 7))
        drained(1, (5, 6, 7))
        drained(2, (5, 6, 7))
        drained(2, (8, 9))

        @pl.when((y == 7) & (row % 8 == 7))
        def _():
            arrived(top.at[parts[0]], top_sem.at[0])
            arrived(top.at[parts[1]], top_sem.at[1])

        @pl.when((y == 7) & (row == 31))
        def _():
            arrived(top.at[parts[2]], top_sem.at[2])

        finish()


def shards(dense_a, dense_b, inner, outer, ascent, descent, couplings):
    dma = pltpu.SemaphoreType.DMA
    tile = (128, 128)
    return pl.pallas_call(
        kernel,
        out_shape=pltpu.VMEM((2, 512, 512), BF),
        in_specs=[pl.BlockSpec(memory_space=pltpu.HBM)] * 7,
        out_specs=pl.BlockSpec(memory_space=pltpu.VMEM),
        scratch_shapes=[
            pltpu.VMEM((2, 512, 512), BF),
            pltpu.VMEM((2, 512, 512), BF),
            pltpu.VMEM((2, 2, 512, 128), BF),
            pltpu.VMEM((2, 2, 512, 128), BF),
            pltpu.VMEM((4, 2, *tile), BF),
            pltpu.VMEM((4, 2, *tile), BF),
            pltpu.VMEM((2, 4, *tile), BF),
            pltpu.VMEM((2, 512, 512), F32),
            pltpu.VMEM((2, 512, 128), BF),
            pltpu.VMEM((2, 512, 128), BF),
            pltpu.VMEM((2, 128, 512), BF),
            pltpu.VMEM((10, *tile), BF),
            pltpu.VMEM((10, *tile), BF),
            pltpu.VMEM((10, *tile), BF),
            pltpu.VMEM((10, *tile), BF),
            pltpu.VMEM((8, 2, *tile), BF),
            pltpu.VMEM((8, 2, *tile), BF),
            pltpu.VMEM((10, 2, *tile), BF),
            pltpu.VMEM((8, *tile), BF),
            pltpu.VMEM((8, *tile), BF),
            pltpu.VMEM((3, 6, *tile), BF),
            pltpu.VMEM((3, *tile), F32),
            pltpu.VMEM((3, *tile), F32),
            dma((11,)),
            dma((10,)),
            dma((10,)),
            dma((10,)),
            dma((8,)),
            dma((8,)),
            dma((10,)),
            dma((1,)),
            dma((3,)),
            dma((3,)),
            dma((3, 3)),
            dma((3,)),
            dma((5, 3)),
            dma((3,)),
            dma((6,)),
            dma,
            dma,
            pltpu.SemaphoreType.REGULAR,
            pltpu.SemaphoreType.REGULAR,
            pltpu.SemaphoreType.REGULAR,
            dma,
        ],
        compiler_params=pltpu.CompilerParams(collective_id=0, has_side_effects=True, vmem_limit_bytes=24 * 2**20),
        name="tree",
    )(*[pltpu.with_memory_space_constraint(v, pltpu.HBM) for v in (dense_a, dense_b, inner, outer, ascent, descent, couplings)])


def solution(mesh):
    placed = (
        P(("row", "col"), None, None),
        P(("row", "col"), None, None),
        P(("row", "col"), None, None, None),
        P(("row", "col"), None, None, None),
        P(("row", "col"), None, None, None, None),
        P(("row", "col"), None, None, None, None),
        P(("row", "col"), None, None, None, None),
    )
    return jax.shard_map(
        shards, mesh=mesh, in_specs=placed, out_specs=P(("row", "col"), None, None), check_vma=False
    )
```
